128 devices in a mesh: group: 4 (over y), tm: 32 (over x, z, core).
Axes of the slice: x: 4, y: 4, z: 4, core: 2. Of those that a mesh axis runs over, the one named last changes fastest.
Arguments:
- precip: bfloat16 [4, 128, 1440, 720], P('group', 'tm'), may hold values from 0.099609375 to 4
- day_bins: int32 [128], replicated, may hold values from 0 to 15
- family_of: int32 [4], replicated, may hold values from 0 to 2
Outputs:
- day_mean: bfloat16 [4, 16, 1440, 720], P('group', None, 'tm')
- day_second: bfloat16 [4, 16, 1440, 720], P('group', None, 'tm')
- day_third: bfloat16 [4, 16, 1440, 720], P('group', None, 'tm')
- family_mean: bfloat16 [3, 16, 1440, 720], P(None, None, 'tm')
- anomaly_norm: float32 [4, 128], replicated
The draws below stay inside these ranges and needn't reach their ends.
All inputs are finite; a program needn't handle non-finite values.
Results may differ from the reference program's by a relative error of at most 0.001.
The reference program's roundings to bfloat16 on the way count: a program that leaves them out, or rounds other values in their place, can miss the bound.
Values may be sent and summed in bfloat16 or wider, within the bound.
No kernel may reach another device: no remote copies, remote signals or barrier semaphores. Data moves between devices by JAX's collectives and lax.ppermute only.
A program may use at most 192 MiB of HBM per device.

```python
import math
import jax
import jax.numpy as jnp
from jax import lax

LON = 1440
LAT = 720
DAYS = 16
FAM = 3
MODELS = 4
TIME = 128


def with_ends(entries, stream_key, least, top_value):
    longest = entries.shape.index(max(entries.shape))
    spots = []
    for shift in (0, 1):
        where = [jax.random.randint(jax.random.fold_in(stream_key, axis), (), 0, length) for axis, length in enumerate(entries.shape)]
        where[longest] = (where[longest] + shift) % entries.shape[longest]
        spots.append(tuple(where))
    return entries.at[spots[0]].set(least).at[spots[1]].set(top_value)


def block_scale(rng, dims, split, smallest, largest):
    def one(axis_at, parts):
        heights = jax.random.uniform(jax.random.fold_in(jax.random.fold_in(rng, 6), axis_at), (parts,), jnp.float32, smallest / len(split), largest / len(split))
        return jnp.repeat(jnp.exp(heights), dims[axis_at] // parts).reshape((-1,) + (1,) * (len(dims) - axis_at - 1))

    factor_of = one(*split[0])
    for cut in split[1:]:
        factor_of = factor_of * one(*cut)
    return factor_of


def setup_inputs(seed: int = 0) -> dict:
    seeds = jax.random.split(jax.random.key(seed), 4)
    return {
        "precip": jnp.clip(jnp.exp(math.log(4.0) - 3.6927934 * jax.random.uniform(seeds[0], (MODELS, TIME, LON, LAT), jnp.float32) ** block_scale(seeds[0], (MODELS, TIME, LON, LAT), ((0, 4), (1, 32)), -0.2, 0.2)), 0.099609375, 4.0).astype(jnp.bfloat16),
        "day_bins": with_ends(jax.random.randint(seeds[1], (TIME,), 0, DAYS), jax.random.fold_in(seeds[1], 1), 0, DAYS - 1).astype(jnp.int32),
        "family_of": with_ends(jax.random.randint(seeds[2], (MODELS,), 0, FAM), jax.random.fold_in(seeds[2], 1), 0, FAM - 1).astype(jnp.int32),
    }


def lat_weight():
    rows_idx = jnp.arange(LAT, dtype=jnp.float32)
    return jnp.cos((-90.0 + (rows_idx + 0.5) * 180.0 / LAT) * (math.pi / 180.0))

def reference(precip, day_bins, family_of):
    onehot = day_bins[None, :] == jnp.arange(DAYS, dtype=jnp.int32)[:, None]
    onehot_f = onehot.astype(jnp.float32)
    divisor = jnp.maximum(lax.optimization_barrier(jnp.sum(onehot_f, axis=1)), 1.0)
    weight = lat_weight()
    total_weight = LON * jnp.sum(weight)

    def one_model(fields):
        flat_cells = fields.reshape(TIME, LON * LAT)
        bin_sums = jnp.dot(onehot.astype(jnp.bfloat16), flat_cells, preferred_element_type=jnp.float32)
        means = bin_sums / divisor[:, None]
        anomaly = flat_cells.astype(jnp.float32) - jnp.take(means, day_bins, axis=0)
        square = anomaly * anomaly
        second = jnp.dot(onehot_f, square, precision=lax.Precision.HIGHEST) / divisor[:, None]
        third = jnp.dot(onehot_f, square * anomaly, precision=lax.Precision.HIGHEST) / divisor[:, None]
        weighted = lax.optimization_barrier(jnp.sum(square.reshape(TIME, LON, LAT) * weight[None, None, :], axis=(1, 2)))
        norm_value = jnp.sqrt(weighted / total_weight)
        shape = (DAYS, LON, LAT)
        return (means.astype(jnp.bfloat16).reshape(shape), second.astype(jnp.bfloat16).reshape(shape), third.astype(jnp.bfloat16).reshape(shape), norm_value)
    day_mean, day_second, day_third, anomaly_norm = lax.map(one_model, precip)
    family_hot = (family_of[None, :] == jnp.arange(FAM, dtype=jnp.int32)[:, None]).astype(jnp.float32)
    family_count = jnp.maximum(lax.optimization_barrier(jnp.sum(family_hot, axis=1)), 1.0)
    summed = jnp.tensordot(family_hot, day_mean.astype(jnp.float32), axes=1, precision=lax.Precision.HIGHEST)
    family_mean = (summed / family_count[:, None, None, None]).astype(jnp.bfloat16)
    return (day_mean, day_second, day_third, family_mean, anomaly_norm)
```

```python
import functools
import math

import jax
import jax.numpy as jnp
import numpy as np
from jax import lax
from jax.experimental import pallas as pl
from jax.experimental.pallas import tpu as pltpu
from jax.sharding import PartitionSpec as P

LON = 1440
LAT = 720
DAYS = 16
FAM = 3
MODELS = 4
TIME = 128
LANES = 128
FULL = LAT // LANES
TAIL = LAT - FULL * LANES
HALF = TAIL // 2
PEERS = 32
BAND = LON // PEERS
BLOCK = 8 * BAND
CHUNKS = (8, 5, 2)

F32 = jnp.float32
BF16 = jnp.bfloat16


def rows_of(triples):
    return -(-17 * triples // 8) * 8


def packed_weight(triples):
    lat = np.arange(LAT, dtype=np.float64)
    weight = np.cos((-90.0 + (lat + 0.5) * 180.0 / LAT) * (math.pi / 180.0))
    count = 3 * triples
    rows = np.zeros((rows_of(triples), LANES))
    for j in range(FULL):
        rows[j * count : (j + 1) * count] = weight[j * LANES : (j + 1) * LANES]
    tail = weight[FULL * LANES :]
    for half in range(2):
        part = rows[FULL * count + half * triples : FULL * count + (half + 1) * triples]
        part[:, :TAIL] = tail
        part[:, TAIL : TAIL + HALF] = tail[half * HALF : (half + 1) * HALF]
    return rows.astype(np.float32), float(weight.sum() * LON)


def pack_kernel(first, triples, x_ref, out_ref, wide, rows):
    count = 3 * triples
    used = 17 * triples
    total = rows_of(triples)
    for j in range(FULL):
        wide[j] = x_ref[0, :, j * LANES : (j + 1) * LANES].astype(F32)
    wide[FULL, :, :TAIL] = x_ref[0, :, FULL * LANES :].astype(F32)
    if total > used:
        rows[total - 8 :, :] = jnp.zeros((8, LANES), F32)
    lane = lax.broadcasted_iota(jnp.int32, (triples, LANES), 1)
    for r in range(8):
        s = BAND * r + first
        for j in range(FULL):
            rows[j * count : (j + 1) * count, :] = wide[j, s : s + count, :]
        third = wide[FULL, s + 2 * triples : s + 3 * triples, :]
        for half in range(2):
            own = wide[FULL, s + half * triples : s + (half + 1) * triples, :]
            moved = pltpu.roll(third, TAIL - half * HALF, 1)
            rows[FULL * count + half * triples : FULL * count + (half + 1) * triples, :] = jnp.where(
                lane < TAIL, own, jnp.where(lane < TAIL + HALF, moved, 0.0)
            )
        out_ref[r, 0] = rows[...].astype(BF16)


def pack(x, first, triples):
    steps = x.shape[0]
    total = rows_of(triples)
    return pl.pallas_call(
        functools.partial(pack_kernel, first, triples),
        grid=(LON // BLOCK, steps),
        in_specs=[pl.BlockSpec((1, BLOCK, LAT), lambda q, t: (t, q, 0))],
        out_specs=pl.BlockSpec((8, 1, total, LANES), lambda q, t: (q, t, 0, 0)),
        out_shape=jax.ShapeDtypeStruct((PEERS, steps, total, LANES), BF16),
        scratch_shapes=[pltpu.VMEM((FULL + 1, BLOCK, LANES), F32), pltpu.VMEM((total, LANES), F32)],
        cost_estimate=pl.CostEstimate(flops=10_000_000, bytes_accessed=12_000_000, transcendentals=0),
        name=f"pack{first}",
    )(x)


def spread(value, day, total, table):
    table[pl.ds(day, total, stride=DAYS), :] = value


def unpack(table, out, triples):
    count = 3 * triples
    lane = lax.broadcasted_iota(jnp.int32, (DAYS, LANES), 1)

    def row(index):
        return table[pl.ds(pl.multiple_of(index * DAYS, DAYS), DAYS), :]

    def whole(lon, carry):
        for j in range(FULL):
            out[lon, :, j * LANES : (j + 1) * LANES] = row(j * count + lon).astype(BF16)
        return carry

    def tail(lon, carry):
        out[lon, :, FULL * LANES :] = row(FULL * count + lon)[:, :TAIL].astype(BF16)
        return carry

    def last(k, carry):
        low = pltpu.roll(row(FULL * count + k), LANES - TAIL, 1)
        high = pltpu.roll(row(FULL * count + triples + k), LANES - TAIL + HALF, 1)
        joined = jnp.where(lane < HALF, low, high)
        out[2 * triples + k, :, FULL * LANES :] = joined[:, :TAIL].astype(BF16)
        return carry

    lax.fori_loop(0, count, whole, 0)
    lax.fori_loop(0, 2 * triples, tail, 0)
    lax.fori_loop(0, triples, last, 0)


def moment_kernel(first, triples, chained, *refs):
    bins, inverse, x, weight, before = refs[:5]
    refs = refs[5 + (3 if chained else 0) :]
    day_mean, day_second, day_third, packed, after, mean, second, third, norm, table, wide, sem = refs
    total = rows_of(triples)
    count = 3 * triples
    tiles = total // 8

    zero = jnp.zeros((total, LANES), F32)
    for d in range(DAYS):
        mean[d] = zero
        second[d] = zero
        third[d] = zero

    def add(t, carry):
        d = bins[t]
        mean[d] = mean[d] + x[t].astype(F32)
        return carry

    lax.fori_loop(0, TIME, add, 0, unroll=4)

    for d in range(DAYS):
        value = mean[d] * inverse[d]
        mean[d] = value
        packed[d] = value.astype(BF16)
        spread(value, d, total, table)
    unpack(table, wide.at[0], triples)

    def moments(t, carry):
        d = bins[t]
        sums = None
        for k in range(tiles):
            at = slice(8 * k, 8 * k + 8)
            a = x[t, at].astype(F32) - mean[d, at]
            q = a * a
            second[d, at] = second[d, at] + q
            third[d, at] = third[d, at] + q * a
            w = q * weight[at]
            sums = w if sums is None else sums + w
        norm[t] = sums
        return carry

    lax.fori_loop(0, TIME, moments, 0, unroll=2)

    for slot, ref in ((1, second), (2, third)):
        for d in range(DAYS):
            spread(ref[d] * inverse[d], d, total, table)
        unpack(table, wide.at[slot], triples)

    by_time = jnp.sum(norm[...], axis=1)
    after[...] = before[...] + jnp.sum(by_time.T, axis=0, keepdims=True)

    copies = [
        pltpu.make_async_copy(wide.at[i], out.at[pl.ds(first, count)], sem.at[i])
        for i, out in enumerate((day_mean, day_second, day_third))
    ]
    for copy in copies:
        copy.start()
    for copy in copies:
        copy.wait()


def moments(bins, inverse, x, weight, before, outs, first, triples):
    total = rows_of(triples)
    count = 3 * triples
    smem = pl.BlockSpec(memory_space=pltpu.SMEM)
    vmem = pl.BlockSpec(memory_space=pltpu.VMEM)
    anywhere = pl.BlockSpec(memory_space=pl.ANY)
    chained = outs is not None
    field = jax.ShapeDtypeStruct((BAND, DAYS, LAT), BF16)
    result = pl.pallas_call(
        functools.partial(moment_kernel, first, triples, chained),
        in_specs=[smem, smem, vmem, vmem, vmem] + [anywhere] * (3 if chained else 0),
        out_specs=[anywhere] * 3 + [vmem, vmem],
        out_shape=[
            field,
            field,
            field,
            jax.ShapeDtypeStruct((DAYS, total, LANES), BF16),
            jax.ShapeDtypeStruct((1, TIME), F32),
        ],
        input_output_aliases={5: 0, 6: 1, 7: 2} if chained else {},
        scratch_shapes=[
            pltpu.VMEM((DAYS, total, LANES), F32),
            pltpu.VMEM((DAYS, total, LANES), F32),
            pltpu.VMEM((DAYS, total, LANES), F32),
            pltpu.VMEM((TIME, 8, LANES), F32),
            pltpu.VMEM((total * DAYS, LANES), F32),
            pltpu.VMEM((3, count, DAYS, LAT), BF16),
            pltpu.SemaphoreType.DMA((3,)),
        ],
        cost_estimate=pl.CostEstimate(flops=40_000_000 * triples, bytes_accessed=1_000_000 * triples, transcendentals=0),
        name=f"moments{first}",
    )(bins, inverse, x, weight, before, *(outs or ()))
    return result[:3], result[3], result[4]


def family_kernel(first, triples, chained, *refs):
    share = refs[0]
    own = refs[1:5]
    out, table, wide, sem = refs[5 + (1 if chained else 0) :]
    total = rows_of(triples)
    count = 3 * triples
    copies = []
    for f in range(FAM):
        for d in range(DAYS):
            value = own[0][d].astype(F32) * share[f, 0]
            for k in range(1, MODELS):
                value = value + own[k][d].astype(F32) * share[f, k]
            spread(value * share[f, MODELS], d, total, table)
        unpack(table, wide.at[f], triples)
        copies.append(pltpu.make_async_copy(wide.at[f], out.at[f, pl.ds(first, count)], sem.at[f]))
        copies[-1].start()
    for copy in copies:
        copy.wait()


def families(share, means, out, first, triples):
    total = rows_of(triples)
    count = 3 * triples
    vmem = pl.BlockSpec(memory_space=pltpu.VMEM)
    anywhere = pl.BlockSpec(memory_space=pl.ANY)
    chained = out is not None
    return pl.pallas_call(
        functools.partial(family_kernel, first, triples, chained),
        in_specs=[pl.BlockSpec(memory_space=pltpu.SMEM)] + [vmem] * MODELS + [anywhere] * (1 if chained else 0),
        out_specs=anywhere,
        out_shape=jax.ShapeDtypeStruct((FAM, BAND, DAYS, LAT), BF16),
        input_output_aliases={5: 0} if chained else {},
        scratch_shapes=[
            pltpu.VMEM((total * DAYS, LANES), F32),
            pltpu.VMEM((FAM, count, DAYS, LAT), BF16),
            pltpu.SemaphoreType.DMA((FAM,)),
        ],
        cost_estimate=pl.CostEstimate(flops=10_000_000 * triples, bytes_accessed=500_000 * triples, transcendentals=0),
        name=f"families{first}",
    )(share, *means, *(() if out is None else (out,)))


def local(precip, day_bins, family_of):
    days = jnp.arange(DAYS, dtype=jnp.int32)
    counts = jnp.sum((day_bins[None, :] == days[:, None]).astype(F32), axis=1)
    inverse = 1.0 / jnp.maximum(counts, 1.0)

    group = lax.axis_index("group")
    turned = (group - jnp.arange(MODELS, dtype=jnp.int32)) % MODELS
    hot = (family_of[None, :] == jnp.arange(FAM, dtype=jnp.int32)[:, None]).astype(F32)
    members = jnp.maximum(jnp.sum(hot, axis=1, keepdims=True), 1.0)
    picked = jnp.sum(
        hot[:, None, :] * (turned[:, None] == jnp.arange(MODELS, dtype=jnp.int32)[None, :]).astype(F32)[None],
        axis=2,
    )
    share = jnp.concatenate([picked, 1.0 / members], axis=1)

    x = precip[0]
    first = 0
    starts = []
    for triples in CHUNKS:
        starts.append(first)
        first += 3 * triples
    sent = [pack(x, s, n) for s, n in zip(starts, CHUNKS)]
    got = [lax.all_to_all(p, "tm", split_axis=0, concat_axis=0, tiled=True) for p in sent]

    outs, fam = None, None
    norm = jnp.zeros((1, TIME), F32)
    for s, n, g in zip(starts, CHUNKS, got):
        weight, total_weight = packed_weight(n)
        outs, mean, norm = moments(
            day_bins, inverse, g.reshape(TIME, rows_of(n), LANES), jnp.asarray(weight), norm, outs, s, n
        )
        means = [mean] + [
            lax.ppermute(mean, "group", [(i, (i + k) % MODELS) for i in range(MODELS)]) for k in range(1, MODELS)
        ]
        fam = families(share, means, fam, s, n)

    mine = jnp.where(jnp.arange(MODELS, dtype=jnp.int32)[:, None] == group, norm, 0.0)
    anomaly_norm = jnp.sqrt(lax.psum(mine, ("group", "tm")) / total_weight)
    fields = [o[None].transpose(0, 2, 1, 3) for o in outs]
    return (*fields, fam.transpose(0, 2, 1, 3), anomaly_norm)


def solution(mesh):
    in_specs = (P("group", "tm", None, None), P(), P())
    out_specs = (
        P("group", None, "tm", None),
        P("group", None, "tm", None),
        P("group", None, "tm", None),
        P(None, None, "tm", None),
        P(),
    )
    return jax.shard_map(local, mesh=mesh, in_specs=in_specs, out_specs=out_specs, check_vma=False)
```

```python
import functools
import math

import jax
import jax.numpy as jnp
import numpy as np
from jax import lax
from jax.experimental import pallas as pl
from jax.experimental.pallas import tpu as pltpu
from jax.sharding import PartitionSpec as P

LON = 1440
LAT = 720
DAYS = 16
FAM = 3
MODELS = 4
TIME = 128
LANES = 128
FULL = LAT // LANES
TAIL = LAT - FULL * LANES
HALF = TAIL // 2
PEERS = 32
BAND = LON // PEERS
BLOCK = 8 * BAND
CHUNKS = (11, 4)

F32 = jnp.float32
BF16 = jnp.bfloat16


def rows_of(triples):
    return -(-17 * triples // 8) * 8


def packed_weight(triples):
    lat = np.arange(LAT, dtype=np.float64)
    weight = np.cos((-90.0 + (lat + 0.5) * 180.0 / LAT) * (math.pi / 180.0))
    count = 3 * triples
    rows = np.zeros((rows_of(triples), LANES))
    for j in range(FULL):
        rows[j * count : (j + 1) * count] = weight[j * LANES : (j + 1) * LANES]
    tail = weight[FULL * LANES :]
    for half in range(2):
        part = rows[FULL * count + half * triples : FULL * count + (half + 1) * triples]
        part[:, :TAIL] = tail
        part[:, TAIL : TAIL + HALF] = tail[half * HALF : (half + 1) * HALF]
    return rows.astype(np.float32), float(weight.sum() * LON)


def pack_kernel(first, triples, steps, x, out, held, ready, wide, rows, got, put):
    count = 3 * triples
    used = 17 * triples
    total = rows_of(triples)
    pieces = LON // BLOCK * steps
    lane = lax.broadcasted_iota(jnp.int32, (triples, LANES), 1)

    def enter(i):
        q, t = i // steps, i % steps
        return pltpu.make_async_copy(x.at[t, pl.ds(pl.multiple_of(q * BLOCK, 8), BLOCK)], held.at[i], got.at[i])

    def leave(i):
        q, t = i // steps, i % steps
        return pltpu.make_async_copy(ready.at[i], out.at[pl.ds(q * 8, 8), t], put.at[i])

    for i in range(pieces):
        enter(i).start()
    if total > used:
        rows[total - 8 :, :] = jnp.zeros((8, LANES), F32)

    def piece(i, carry):
        enter(i).wait()
        for j in range(FULL):
            wide[j] = held[i, :, j * LANES : (j + 1) * LANES].astype(F32)
        wide[FULL, :, :TAIL] = held[i, :, FULL * LANES :].astype(F32)
        for r in range(8):
            s = BAND * r + first
            for j in range(FULL):
                rows[j * count : (j + 1) * count, :] = wide[j, s : s + count, :]
            third = wide[FULL, s + 2 * triples : s + 3 * triples, :]
            for half in range(2):
                own = wide[FULL, s + half * triples : s + (half + 1) * triples, :]
                moved = pltpu.roll(third, TAIL - half * HALF, 1)
                rows[FULL * count + half * triples : FULL * count + (half + 1) * triples, :] = jnp.where(
                    lane < TAIL, own, jnp.where(lane < TAIL + HALF, moved, 0.0)
                )
            ready[i, r] = rows[...].astype(BF16)
        leave(i).start()
        return carry

    lax.fori_loop(0, pieces, piece, 0)
    for i in range(pieces):
        leave(i).wait()


def pack(x, first, triples):
    steps = x.shape[0]
    total = rows_of(triples)
    pieces = LON // BLOCK * steps
    return pl.pallas_call(
        functools.partial(pack_kernel, first, triples, steps),
        in_specs=[pl.BlockSpec(memory_space=pl.ANY)],
        out_specs=pl.BlockSpec(memory_space=pl.ANY),
        out_shape=jax.ShapeDtypeStruct((PEERS, steps, total, LANES), BF16),
        scratch_shapes=[
            pltpu.VMEM((pieces, BLOCK, LAT), BF16),
            pltpu.VMEM((pieces, 8, total, LANES), BF16),
            pltpu.VMEM((FULL + 1, BLOCK, LANES), F32),
            pltpu.VMEM((total, LANES), F32),
            pltpu.SemaphoreType.DMA((pieces,)),
            pltpu.SemaphoreType.DMA((pieces,)),
        ],
        cost_estimate=pl.CostEstimate(flops=10_000_000, bytes_accessed=12_000_000, transcendentals=0),
        name=f"pack{first}",
    )(x)


def unpack(table, scale, out, triples):
    stride = rows_of(triples) + 1
    count = 3 * triples
    lane = lax.broadcasted_iota(jnp.int32, (DAYS, LANES), 1)

    def row(index):
        halves = [table[pl.ds(8 * h * stride + index, 8, stride=stride), :] for h in range(DAYS // 8)]
        value = jnp.concatenate(halves, axis=0)
        return value if scale is None else value * scale

    def whole(lon, carry):
        for j in range(FULL):
            out[lon, :, j * LANES : (j + 1) * LANES] = row(j * count + lon).astype(BF16)
        return carry

    def tail(lon, carry):
        out[lon, :, FULL * LANES :] = row(FULL * count + lon)[:, :TAIL].astype(BF16)
        return carry

    def last(k, carry):
        low = pltpu.roll(row(FULL * count + k), LANES - TAIL, 1)
        high = pltpu.roll(row(FULL * count + triples + k), LANES - TAIL + HALF, 1)
        joined = jnp.where(lane < HALF, low, high)
        out[2 * triples + k, :, FULL * LANES :] = joined[:, :TAIL].astype(BF16)
        return carry

    lax.fori_loop(0, count, whole, 0)
    lax.fori_loop(0, 2 * triples, tail, 0)
    lax.fori_loop(0, triples, last, 0)


SMEM = pl.BlockSpec(memory_space=pltpu.SMEM)
VMEM = pl.BlockSpec(memory_space=pltpu.VMEM)
ANY = pl.BlockSpec(memory_space=pl.ANY)
STEPS = 4
SPAN = TIME // STEPS


def sum_kernel(triples, bins, inverse, x, mean, packed):
    total = rows_of(triples)
    stride = total + 1
    step = pl.program_id(0)

    @pl.when(step == 0)
    def _():
        for d in range(DAYS):
            mean[d * stride : (d + 1) * stride, :] = jnp.zeros((stride, LANES), F32)

    def add(t, carry):
        at = bins[step * SPAN + t] * stride
        for k in range(total // 8):
            rows = pl.ds(at + 8 * k, 8)
            mean[rows, :] = mean[rows, :] + x[t, 8 * k : 8 * k + 8].astype(F32)
        return carry

    lax.fori_loop(0, SPAN, add, 0, unroll=4)

    @pl.when(step == STEPS - 1)
    def _():
        for d in range(DAYS):
            rows = slice(d * stride, d * stride + total)
            value = mean[rows, :] * inverse[d]
            mean[rows, :] = value
            packed[d] = value.astype(BF16)


def sums(bins, inverse, x, triples):
    total = rows_of(triples)
    return pl.pallas_call(
        functools.partial(sum_kernel, triples),
        grid=(STEPS,),
        in_specs=[SMEM, SMEM, pl.BlockSpec((SPAN, total, LANES), lambda i: (i, 0, 0))],
        out_specs=[
            pl.BlockSpec((DAYS * (total + 1), LANES), lambda i: (0, 0)),
            pl.BlockSpec((DAYS, total, LANES), lambda i: (0, 0, 0)),
        ],
        out_shape=[
            jax.ShapeDtypeStruct((DAYS * (total + 1), LANES), F32),
            jax.ShapeDtypeStruct((DAYS, total, LANES), BF16),
        ],
        cost_estimate=pl.CostEstimate(flops=10_000_000 * triples, bytes_accessed=700_000 * triples, transcendentals=0),
        name=f"sums{triples}",
    )(bins, inverse, x)


def moment_kernel(first, triples, chained, *refs):
    bins, x, mean, inverse, weight, before = refs[:6]
    refs = refs[6 + (3 if chained else 0) :]
    day_mean, day_second, day_third, after, second, third, norm, wide, sem = refs
    total = rows_of(triples)
    stride = total + 1
    count = 3 * triples
    step = pl.program_id(0)
    outs = (day_mean, day_second, day_third)

    def leave(i):
        return pltpu.make_async_copy(wide.at[i], outs[i].at[pl.ds(first, count)], sem.at[i])

    @pl.when(step == 0)
    def _():
        for d in range(DAYS):
            second[d * stride : (d + 1) * stride, :] = jnp.zeros((stride, LANES), F32)
            third[d * stride : (d + 1) * stride, :] = jnp.zeros((stride, LANES), F32)
        unpack(mean, None, wide.at[0], triples)
        leave(0).start()

    def moments(t, carry):
        at = bins[step * SPAN + t] * stride
        sums = None
        for k in range(total // 8):
            rows = pl.ds(at + 8 * k, 8)
            tile = slice(8 * k, 8 * k + 8)
            a = x[t, tile].astype(F32) - mean[rows, :]
            q = a * a
            second[rows, :] = second[rows, :] + q
            third[rows, :] = third[rows, :] + q * a
            w = q * weight[tile, :]
            sums = w if sums is None else sums + w
        norm[step * SPAN + t] = sums
        return carry

    lax.fori_loop(0, SPAN, moments, 0, unroll=2)

    @pl.when(step == STEPS - 1)
    def _():
        by_time = jnp.sum(norm[...], axis=1)
        after[...] = before[...] + jnp.sum(by_time.T, axis=0, keepdims=True)
        scale = inverse[...]
        unpack(second, scale, wide.at[1], triples)
        leave(1).start()
        unpack(third, scale, wide.at[2], triples)
        leave(2).start()
        for i in range(3):
            leave(i).wait()


def moments(bins, inverse, x, mean, weight, before, outs, first, triples):
    total = rows_of(triples)
    count = 3 * triples
    chained = outs is not None
    field = jax.ShapeDtypeStruct((BAND, DAYS, LAT), BF16)
    result = pl.pallas_call(
        functools.partial(moment_kernel, first, triples, chained),
        grid=(STEPS,),
        in_specs=[SMEM, pl.BlockSpec((SPAN, total, LANES), lambda i: (i, 0, 0))]
        + [VMEM] * 4
        + [ANY] * (3 if chained else 0),
        out_specs=[ANY] * 3 + [VMEM],
        out_shape=[field, field, field, jax.ShapeDtypeStruct((1, TIME), F32)],
        input_output_aliases={6: 0, 7: 1, 8: 2} if chained else {},
        scratch_shapes=[
            pltpu.VMEM((DAYS * (total + 1), LANES), F32),
            pltpu.VMEM((DAYS * (total + 1), LANES), F32),
            pltpu.VMEM((TIME, 8, LANES), F32),
            pltpu.VMEM((3, count, DAYS, LAT), BF16),
            pltpu.SemaphoreType.DMA((3,)),
        ],
        cost_estimate=pl.CostEstimate(flops=40_000_000 * triples, bytes_accessed=1_000_000 * triples, transcendentals=0),
        name=f"moments{first}",
    )(bins, x, mean, inverse, weight, before, *(outs or ()))
    return result[:3], result[3]


def family_kernel(first, triples, chained, *refs):
    share, own, right, left, low, high = refs[:6]
    out, table, wide, sem = refs[6 + (1 if chained else 0) :]
    total = rows_of(triples)
    stride = total + 1
    count = 3 * triples
    for d in range(DAYS):
        across = low[d] if d < DAYS // 2 else high[d - DAYS // 2]
        values = [v.astype(F32) for v in (own[d], right[d], left[d], across)]
        for f in range(FAM):
            value = values[0] * share[f, 0]
            for k in range(1, MODELS):
                value = value + values[k] * share[f, k]
            table[f, d * stride : d * stride + total, :] = value
    copies = []
    for f in range(FAM):
        unpack(table.at[f], None, wide.at[f], triples)
        copies.append(pltpu.make_async_copy(wide.at[f], out.at[f, pl.ds(first, count)], sem.at[f]))
        copies[-1].start()
    for copy in copies:
        copy.wait()


def families(share, means, out, first, triples):
    total = rows_of(triples)
    count = 3 * triples
    chained = out is not None
    return pl.pallas_call(
        functools.partial(family_kernel, first, triples, chained),
        in_specs=[SMEM] + [VMEM] * 5 + [ANY] * (1 if chained else 0),
        out_specs=ANY,
        out_shape=jax.ShapeDtypeStruct((FAM, BAND, DAYS, LAT), BF16),
        input_output_aliases={6: 0} if chained else {},
        scratch_shapes=[
            pltpu.VMEM((FAM, DAYS * (total + 1), LANES), F32),
            pltpu.VMEM((FAM, count, DAYS, LAT), BF16),
            pltpu.SemaphoreType.DMA((FAM,)),
        ],
        cost_estimate=pl.CostEstimate(flops=10_000_000 * triples, bytes_accessed=500_000 * triples, transcendentals=0),
        name=f"families{first}",
    )(share, *means, *(() if out is None else (out,)))


def from_others(mean):
    up = [(i, (i + 1) % MODELS) for i in range(MODELS)]
    down = [(i, (i - 1) % MODELS) for i in range(MODELS)]
    behind = lax.ppermute(mean, "group", up)
    ahead = lax.ppermute(mean, "group", down)
    low = lax.ppermute(behind[: DAYS // 2], "group", up)
    high = lax.ppermute(ahead[DAYS // 2 :], "group", down)
    return behind, ahead, low, high


def local(precip, day_bins, family_of):
    days = jnp.arange(DAYS, dtype=jnp.int32)
    counts = jnp.sum((day_bins[None, :] == days[:, None]).astype(F32), axis=1)
    inverse = 1.0 / jnp.maximum(counts, 1.0)
    inverse_rows = jnp.broadcast_to(inverse[:, None], (DAYS, LANES))

    group = lax.axis_index("group")
    turned = (group + jnp.array([0, MODELS - 1, 1, 2], dtype=jnp.int32)) % MODELS
    models = jnp.arange(MODELS, dtype=jnp.int32)
    hot = (family_of[None, :] == jnp.arange(FAM, dtype=jnp.int32)[:, None]).astype(F32)
    members = jnp.maximum(jnp.sum(hot, axis=1), 1.0)
    at = (turned[:, None] == models[None, :]).astype(F32)
    share = jnp.sum(hot[:, None, :] * at[None], axis=2) / members[:, None]

    x = precip[0]
    first = 0
    starts = []
    for triples in CHUNKS:
        starts.append(first)
        first += 3 * triples
    sent = [pack(x, s, n) for s, n in zip(starts, CHUNKS)]
    got = [lax.all_to_all(p, "tm", split_axis=0, concat_axis=0, tiled=True) for p in sent]

    outs, fam = None, None
    norm = jnp.zeros((1, TIME), F32)
    for s, n, g in zip(starts, CHUNKS, got):
        weight, total_weight = packed_weight(n)
        g = g.reshape(TIME, rows_of(n), LANES)
        mean, packed = sums(day_bins, inverse, g, n)
        means = (packed, *from_others(packed))
        outs, norm = moments(day_bins, inverse_rows, g, mean, jnp.asarray(weight), norm, outs, s, n)
        fam = families(share, means, fam, s, n)

    everyone = MODELS * PEERS
    parts = lax.all_to_all(
        jnp.broadcast_to(norm, (everyone, 1, TIME)), ("group", "tm"), split_axis=0, concat_axis=0, tiled=True
    )
    anomaly_norm = jnp.sqrt(jnp.sum(parts.reshape(MODELS, PEERS, TIME), axis=1) / total_weight)
    fields = [o[None].transpose(0, 2, 1, 3) for o in outs]
    return (*fields, fam.transpose(0, 2, 1, 3), anomaly_norm)


def solution(mesh):
    in_specs = (P("group", "tm", None, None), P(), P())
    out_specs = (
        P("group", None, "tm", None),
        P("group", None, "tm", None),
        P("group", None, "tm", None),
        P(None, None, "tm", None),
        P(),
    )
    return jax.shard_map(local, mesh=mesh, in_specs=in_specs, out_specs=out_specs, check_vma=False)
```

```python
import functools
import math

import jax
import jax.numpy as jnp
import numpy as np
from jax import lax
from jax.experimental import pallas as pl
from jax.experimental.pallas import tpu as pltpu
from jax.sharding import PartitionSpec as P


LON = 1440
LAT = 720
DAYS = 16
FAM = 3
MODELS = 4
TIME = 128
LANES = 128
FULL = LAT // LANES
TAIL = LAT - FULL * LANES
HALF = TAIL // 2
PEERS = 32
BAND = LON // PEERS
BLOCK = 8 * BAND
CHUNKS = (11, 4)
STARTS = tuple(3 * sum(CHUNKS[:c]) for c in range(len(CHUNKS)))

SMEM = pl.BlockSpec(memory_space=pltpu.SMEM)
VMEM = pl.BlockSpec(memory_space=pltpu.VMEM)
ANY = pl.BlockSpec(memory_space=pl.ANY)
STEPS = 8
SPAN = TIME // STEPS

F32 = jnp.float32
BF16 = jnp.bfloat16


def rows_of(triples):
    return -(-17 * triples // 8) * 8


def packed_weight(triples):
    lat = np.arange(LAT, dtype=np.float64)
    weight = np.cos((-90.0 + (lat + 0.5) * 180.0 / LAT) * (math.pi / 180.0))
    count = 3 * triples
    rows = np.zeros((rows_of(triples), LANES))
    for j in range(FULL):
        rows[j * count : (j + 1) * count] = weight[j * LANES : (j + 1) * LANES]
    tail = weight[FULL * LANES :]
    for half in range(2):
        part = rows[FULL * count + half * triples : FULL * count + (half + 1) * triples]
        part[:, :TAIL] = tail
        part[:, TAIL : TAIL + HALF] = tail[half * HALF : (half + 1) * HALF]
    return rows.astype(np.float32), float(weight.sum() * LON)


def pack_rows(first, triples, wide, rows, ready):
    count = 3 * triples
    lane = lax.broadcasted_iota(jnp.int32, (triples, LANES), 1)
    for r in range(8):
        s = BAND * r + first
        for j in range(FULL):
            rows[j * count : (j + 1) * count, :] = wide[j, s : s + count, :]
        third = wide[FULL, s + 2 * triples : s + 3 * triples, :]
        for half in range(2):
            own = wide[FULL, s + half * triples : s + (half + 1) * triples, :]
            moved = pltpu.roll(third, TAIL - half * HALF, 1)
            rows[FULL * count + half * triples : FULL * count + (half + 1) * triples, :] = jnp.where(
                lane < TAIL, own, jnp.where(lane < TAIL + HALF, moved, 0.0)
            )
        ready[r] = rows[...].astype(BF16)


def pack_kernel(steps, x, *refs):
    n = len(CHUNKS)
    outs, held, ready, wide = refs[:n], refs[n], refs[n + 1 : 2 * n + 1], refs[2 * n + 1]
    rows, got, put = refs[2 * n + 2 : 3 * n + 2], refs[3 * n + 2], refs[3 * n + 3]
    pieces = LON // BLOCK * steps

    def enter(i):
        q, t = i // steps, i % steps
        return pltpu.make_async_copy(x.at[t, pl.ds(pl.multiple_of(q * BLOCK, 8), BLOCK)], held.at[i], got.at[i])

    def leave(c, i):
        q, t = i // steps, i % steps
        return pltpu.make_async_copy(ready[c].at[i], outs[c].at[pl.ds(q * 8, 8), t], put.at[c, i])

    for i in range(pieces):
        enter(i).start()
    for c, triples in enumerate(CHUNKS):
        total = rows_of(triples)
        rows[c][total - 8 :, :] = jnp.zeros((8, LANES), F32)

    def piece(i, carry):
        enter(i).wait()
        for j in range(FULL):
            wide[j] = held[i, :, j * LANES : (j + 1) * LANES].astype(F32)
        wide[FULL, :, :TAIL] = held[i, :, FULL * LANES :].astype(F32)
        for c, triples in enumerate(CHUNKS):
            pack_rows(STARTS[c], triples, wide, rows[c], ready[c].at[i])
            leave(c, i).start()
        return carry

    lax.fori_loop(0, pieces, piece, 0)
    for c in range(n):
        for i in range(pieces):
            leave(c, i).wait()


def pack(x):
    steps = x.shape[0]
    totals = [rows_of(n) for n in CHUNKS]
    pieces = LON // BLOCK * steps
    return pl.pallas_call(
        functools.partial(pack_kernel, steps),
        in_specs=[ANY],
        out_specs=[ANY] * len(CHUNKS),
        out_shape=[jax.ShapeDtypeStruct((PEERS, steps, total, LANES), BF16) for total in totals],
        scratch_shapes=[pltpu.VMEM((pieces, BLOCK, LAT), BF16)]
        + [pltpu.VMEM((pieces, 8, total, LANES), BF16) for total in totals]
        + [pltpu.VMEM((FULL + 1, BLOCK, LANES), F32)]
        + [pltpu.VMEM((total, LANES), F32) for total in totals]
        + [pltpu.SemaphoreType.DMA((pieces,)), pltpu.SemaphoreType.DMA((len(CHUNKS), pieces))],
        cost_estimate=pl.CostEstimate(flops=10_000_000, bytes_accessed=17_000_000, transcendentals=0),
        name="pack",
    )(x)


def unpack(table, scale, out, triples):
    stride = rows_of(triples) + 1
    count = 3 * triples
    lane = lax.broadcasted_iota(jnp.int32, (DAYS, LANES), 1)

    def row(index):
        halves = [table[pl.ds(8 * h * stride + index, 8, stride=stride), :] for h in range(DAYS // 8)]
        value = jnp.concatenate(halves, axis=0)
        return value if scale is None else value * scale

    def whole(lon, carry):
        for j in range(FULL):
            out[lon, :, j * LANES : (j + 1) * LANES] = row(j * count + lon).astype(BF16)
        return carry

    def tail(lon, carry):
        out[lon, :, FULL * LANES :] = row(FULL * count + lon)[:, :TAIL].astype(BF16)
        return carry

    def last(k, carry):
        low = pltpu.roll(row(FULL * count + k), LANES - TAIL, 1)
        high = pltpu.roll(row(FULL * count + triples + k), LANES - TAIL + HALF, 1)
        joined = jnp.where(lane < HALF, low, high)
        out[2 * triples + k, :, FULL * LANES :] = joined[:, :TAIL].astype(BF16)
        return carry

    lax.fori_loop(0, count, whole, 0)
    lax.fori_loop(0, 2 * triples, tail, 0)
    lax.fori_loop(0, triples, last, 0)


def moment_kernel(first, triples, chained, *refs):
    bins, inverse, x, scale, weight, before = refs[:6]
    refs = refs[6 + (3 if chained else 0) :]
    outs, refs = refs[:3], refs[3:]
    packed, after, held, mean, second, third, norm, wide, got, put = refs
    total = rows_of(triples)
    stride = total + 1
    count = 3 * triples

    def enter(i):
        span = pl.ds(i * SPAN, SPAN)
        return pltpu.make_async_copy(x.at[span], held.at[span], got.at[i])

    def leave(i):
        return pltpu.make_async_copy(wide.at[i], outs[i].at[pl.ds(first, count)], put.at[i])

    for i in range(STEPS):
        enter(i).start()
    for ref in (mean, second, third):
        for d in range(DAYS):
            ref[d * stride : (d + 1) * stride, :] = jnp.zeros((stride, LANES), F32)

    def add(t, carry):
        at = bins[t] * stride
        for k in range(total // 8):
            rows = pl.ds(at + 8 * k, 8)
            mean[rows, :] = mean[rows, :] + held[t, 8 * k : 8 * k + 8].astype(F32)
        return carry

    def adds(i, carry):
        enter(i).wait()
        return lax.fori_loop(0, SPAN, lambda t, c: add(i * SPAN + t, c), carry, unroll=4)

    lax.fori_loop(0, STEPS, adds, 0)

    for d in range(DAYS):
        rows = slice(d * stride, d * stride + total)
        value = mean[rows, :] * inverse[d]
        mean[rows, :] = value
        packed[d] = value.astype(BF16)
    unpack(mean, None, wide.at[0], triples)
    leave(0).start()

    def moments(t, carry):
        at = bins[t] * stride
        sums = None
        for k in range(total // 8):
            rows = pl.ds(at + 8 * k, 8)
            tile = slice(8 * k, 8 * k + 8)
            a = held[t, tile].astype(F32) - mean[rows, :]
            q = a * a
            second[rows, :] = second[rows, :] + q
            third[rows, :] = third[rows, :] + q * a
            w = q * weight[tile, :]
            sums = w if sums is None else sums + w
        norm[t] = sums
        return carry

    lax.fori_loop(0, TIME, moments, 0, unroll=2)

    by_time = jnp.sum(norm[...], axis=1)
    after[...] = before[...] + jnp.sum(by_time.T, axis=0, keepdims=True)
    unpack(second, scale[...], wide.at[1], triples)
    leave(1).start()
    unpack(third, scale[...], wide.at[2], triples)
    leave(2).start()
    for i in range(3):
        leave(i).wait()


def moments(bins, inverse, x, scale, weight, before, outs, first, triples):
    total = rows_of(triples)
    count = 3 * triples
    chained = outs is not None
    field = jax.ShapeDtypeStruct((BAND, DAYS, LAT), BF16)
    table = pltpu.VMEM((DAYS * (total + 1), LANES), F32)
    result = pl.pallas_call(
        functools.partial(moment_kernel, first, triples, chained),
        in_specs=[SMEM, SMEM, ANY, VMEM, VMEM, VMEM] + [ANY] * (3 if chained else 0),
        out_specs=[ANY] * 3 + [VMEM] * 2,
        out_shape=[
            field,
            field,
            field,
            jax.ShapeDtypeStruct((DAYS, total, LANES), BF16),
            jax.ShapeDtypeStruct((1, TIME), F32),
        ],
        input_output_aliases={6: 0, 7: 1, 8: 2} if chained else {},
        scratch_shapes=[
            pltpu.VMEM((TIME, total, LANES), BF16),
            table,
            table,
            table,
            pltpu.VMEM((TIME, 8, LANES), F32),
            pltpu.VMEM((3, count, DAYS, LAT), BF16),
            pltpu.SemaphoreType.DMA((STEPS,)),
            pltpu.SemaphoreType.DMA((3,)),
        ],
        cost_estimate=pl.CostEstimate(flops=40_000_000 * triples, bytes_accessed=1_000_000 * triples, transcendentals=0),
    )(bins, inverse, x, scale, weight, before, *(outs or ()))
    return result[:3], result[3], result[4]


def family_kernel(first, triples, chained, *refs):
    share, *means = refs[: MODELS + 1]
    out, table, wide, sem = refs[MODELS + 1 + (1 if chained else 0) :]
    total = rows_of(triples)
    stride = total + 1
    count = 3 * triples
    for d in range(DAYS):
        values = [m[d].astype(F32) for m in means]
        for f in range(FAM):
            value = values[0] * share[f, 0]
            for k in range(1, MODELS):
                value = value + values[k] * share[f, k]
            table[f, d * stride : d * stride + total, :] = value
    copies = []
    for f in range(FAM):
        unpack(table.at[f], None, wide.at[f], triples)
        copies.append(pltpu.make_async_copy(wide.at[f], out.at[f, pl.ds(first, count)], sem.at[f]))
        copies[-1].start()
    for copy in copies:
        copy.wait()


def families(share, means, out, first, triples):
    total = rows_of(triples)
    count = 3 * triples
    chained = out is not None
    return pl.pallas_call(
        functools.partial(family_kernel, first, triples, chained),
        in_specs=[SMEM] + [VMEM] * MODELS + [ANY] * (1 if chained else 0),
        out_specs=ANY,
        out_shape=jax.ShapeDtypeStruct((FAM, BAND, DAYS, LAT), BF16),
        input_output_aliases={MODELS + 1: 0} if chained else {},
        scratch_shapes=[
            pltpu.VMEM((FAM, DAYS * (total + 1), LANES), F32),
            pltpu.VMEM((FAM, count, DAYS, LAT), BF16),
            pltpu.SemaphoreType.DMA((FAM,)),
        ],
        cost_estimate=pl.CostEstimate(flops=10_000_000 * triples, bytes_accessed=500_000 * triples, transcendentals=0),
    )(share, *means, *(() if out is None else (out,)))


def from_others(mean):
    return [lax.ppermute(mean, "group", [(i, (i + k) % MODELS) for i in range(MODELS)]) for k in range(1, MODELS)]


def exchange(array):
    return lax.all_to_all(array, "tm", split_axis=0, concat_axis=0, tiled=True)


def local(precip, day_bins, family_of):
    sent = pack(precip[0])
    got0, later, day_bins, family_of = lax.optimization_barrier((exchange(sent[0]), sent[1], day_bins, family_of))
    got1 = exchange(later)

    days = jnp.arange(DAYS, dtype=jnp.int32)
    counts = jnp.sum((day_bins[None, :] == days[:, None]).astype(F32), axis=1)
    inverse = 1.0 / jnp.maximum(counts, 1.0)
    scale = jnp.broadcast_to(inverse[:, None], (DAYS, LANES))

    group = lax.axis_index("group")
    turned = (group + MODELS - jnp.arange(MODELS, dtype=jnp.int32)) % MODELS
    models = jnp.arange(MODELS, dtype=jnp.int32)
    hot = (family_of[None, :] == jnp.arange(FAM, dtype=jnp.int32)[:, None]).astype(F32)
    members = jnp.maximum(jnp.sum(hot, axis=1), 1.0)
    at = (turned[:, None] == models[None, :]).astype(F32)
    share = jnp.sum(hot[:, None, :] * at[None], axis=2) / members[:, None]

    def chunk(c, got, norm, outs):
        weight, _ = packed_weight(CHUNKS[c])
        x = got.reshape(TIME, rows_of(CHUNKS[c]), LANES)
        return moments(day_bins, inverse, x, scale, jnp.asarray(weight), norm, outs, STARTS[c], CHUNKS[c])

    outs, mean0, norm = chunk(0, got0, jnp.zeros((1, TIME), F32), None)
    means0 = [mean0, *from_others(mean0)]
    got1, outs = lax.optimization_barrier((got1, outs))
    outs, mean1, norm = chunk(1, got1, norm, outs)
    means1 = [mean1, *from_others(mean1)]

    everyone = MODELS * PEERS
    parts = lax.all_to_all(
        jnp.broadcast_to(norm, (everyone, 1, TIME)), ("group", "tm"), split_axis=0, concat_axis=0, tiled=True
    )
    fam = families(share, means0, None, STARTS[0], CHUNKS[0])
    fam = families(share, means1, fam, STARTS[1], CHUNKS[1])

    _, total_weight = packed_weight(CHUNKS[0])
    anomaly_norm = jnp.sqrt(jnp.sum(parts.reshape(MODELS, PEERS, TIME), axis=1) / total_weight)
    fields = [o[None].transpose(0, 2, 1, 3) for o in outs]
    return (*fields, fam.transpose(0, 2, 1, 3), anomaly_norm)


def solution(mesh):
    in_specs = (P("group", "tm", None, None), P(), P())
    out_specs = (
        P("group", None, "tm", None),
        P("group", None, "tm", None),
        P("group", None, "tm", None),
        P(None, None, "tm", None),
        P(),
    )
    return jax.shard_map(local, mesh=mesh, in_specs=in_specs, out_specs=out_specs, check_vma=False)
```

```python
import functools
import math

import jax
import jax.numpy as jnp
import numpy as np
from jax import lax
from jax.experimental import pallas as pl
from jax.experimental.pallas import tpu as pltpu
from jax.sharding import PartitionSpec as P


LON = 1440
LAT = 720
DAYS = 16
FAM = 3
MODELS = 4
TIME = 128
LANES = 128
FULL = LAT // LANES
TAIL = LAT - FULL * LANES
HALF = TAIL // 2
PEERS = 32
BAND = LON // PEERS
BLOCK = 8 * BAND
CHUNKS = (11, 4)
STARTS = tuple(3 * sum(CHUNKS[:c]) for c in range(len(CHUNKS)))

SMEM = pl.BlockSpec(memory_space=pltpu.SMEM)
VMEM = pl.BlockSpec(memory_space=pltpu.VMEM)
ANY = pl.BlockSpec(memory_space=pl.ANY)
STEPS = 8
SPARE = 94_000
SPAN = TIME // STEPS

F32 = jnp.float32
BF16 = jnp.bfloat16


def rows_of(triples):
    return -(-17 * triples // 8) * 8


def packed_weight(triples):
    lat = np.arange(LAT, dtype=np.float64)
    weight = np.cos((-90.0 + (lat + 0.5) * 180.0 / LAT) * (math.pi / 180.0))
    count = 3 * triples
    rows = np.zeros((rows_of(triples), LANES))
    for j in range(FULL):
        rows[j * count : (j + 1) * count] = weight[j * LANES : (j + 1) * LANES]
    tail = weight[FULL * LANES :]
    for half in range(2):
        part = rows[FULL * count + half * triples : FULL * count + (half + 1) * triples]
        part[:, :TAIL] = tail
        part[:, TAIL : TAIL + HALF] = tail[half * HALF : (half + 1) * HALF]
    return rows.astype(np.float32), float(weight.sum() * LON)


def pack_rows(first, triples, wide, rows, ready):
    count = 3 * triples
    lane = lax.broadcasted_iota(jnp.int32, (triples, LANES), 1)
    for r in range(8):
        s = BAND * r + first
        for j in range(FULL):
            rows[j * count : (j + 1) * count, :] = wide[j, s : s + count, :]
        third = wide[FULL, s + 2 * triples : s + 3 * triples, :]
        for half in range(2):
            own = wide[FULL, s + half * triples : s + (half + 1) * triples, :]
            moved = pltpu.roll(third, TAIL - half * HALF, 1)
            rows[FULL * count + half * triples : FULL * count + (half + 1) * triples, :] = jnp.where(
                lane < TAIL, own, jnp.where(lane < TAIL + HALF, moved, 0.0)
            )
        ready[r] = rows[...].astype(BF16)


def pack_kernel(steps, x, *refs):
    n = len(CHUNKS)
    outs, held, ready, wide = refs[:n], refs[n], refs[n + 1 : 2 * n + 1], refs[2 * n + 1]
    rows, got, put = refs[2 * n + 2 : 3 * n + 2], refs[3 * n + 2], refs[3 * n + 3]
    pieces = LON // BLOCK * steps

    def enter(i):
        q, t = i // steps, i % steps
        return pltpu.make_async_copy(x.at[t, pl.ds(pl.multiple_of(q * BLOCK, 8), BLOCK)], held.at[i], got.at[i])

    def leave(c, i):
        q, t = i // steps, i % steps
        return pltpu.make_async_copy(ready[c].at[i], outs[c].at[pl.ds(q * 8, 8), t], put.at[c, i])

    for i in range(pieces):
        enter(i).start()
    for c, triples in enumerate(CHUNKS):
        total = rows_of(triples)
        rows[c][total - 8 :, :] = jnp.zeros((8, LANES), F32)

    def piece(i, carry):
        enter(i).wait()
        for j in range(FULL):
            wide[j] = held[i, :, j * LANES : (j + 1) * LANES].astype(F32)
        wide[FULL, :, :TAIL] = held[i, :, FULL * LANES :].astype(F32)
        for c, triples in enumerate(CHUNKS):
            pack_rows(STARTS[c], triples, wide, rows[c], ready[c].at[i])
            leave(c, i).start()
        return carry

    lax.fori_loop(0, pieces, piece, 0)
    for c in range(n):
        for i in range(pieces):
            leave(c, i).wait()


def pack(x):
    steps = x.shape[0]
    totals = [rows_of(n) for n in CHUNKS]
    pieces = LON // BLOCK * steps
    return pl.pallas_call(
        functools.partial(pack_kernel, steps),
        in_specs=[ANY],
        out_specs=[ANY] * len(CHUNKS),
        out_shape=[jax.ShapeDtypeStruct((PEERS, steps, total, LANES), BF16) for total in totals],
        scratch_shapes=[pltpu.VMEM((pieces, BLOCK, LAT), BF16)]
        + [pltpu.VMEM((pieces, 8, total, LANES), BF16) for total in totals]
        + [pltpu.VMEM((FULL + 1, BLOCK, LANES), F32)]
        + [pltpu.VMEM((total, LANES), F32) for total in totals]
        + [pltpu.SemaphoreType.DMA((pieces,)), pltpu.SemaphoreType.DMA((len(CHUNKS), pieces))],
        cost_estimate=pl.CostEstimate(flops=10_000_000, bytes_accessed=17_000_000, transcendentals=0),
        name="pack",
    )(x)


def unpack(table, scale, out, triples):
    stride = rows_of(triples) + 1
    count = 3 * triples
    lane = lax.broadcasted_iota(jnp.int32, (DAYS, LANES), 1)

    def row(index):
        halves = [table[pl.ds(8 * h * stride + index, 8, stride=stride), :] for h in range(DAYS // 8)]
        value = jnp.concatenate(halves, axis=0)
        return value if scale is None else value * scale

    def whole(lon, carry):
        for j in range(FULL):
            out[lon, :, j * LANES : (j + 1) * LANES] = row(j * count + lon).astype(BF16)
        return carry

    def tail(lon, carry):
        out[lon, :, FULL * LANES :] = row(FULL * count + lon)[:, :TAIL].astype(BF16)
        return carry

    def last(k, carry):
        low = pltpu.roll(row(FULL * count + k), LANES - TAIL, 1)
        high = pltpu.roll(row(FULL * count + triples + k), LANES - TAIL + HALF, 1)
        joined = jnp.where(lane < HALF, low, high)
        out[2 * triples + k, :, FULL * LANES :] = joined[:, :TAIL].astype(BF16)
        return carry

    lax.fori_loop(0, count, whole, 0, unroll=3)
    lax.fori_loop(0, 2 * triples, tail, 0, unroll=2)
    lax.fori_loop(0, triples, last, 0)


def zero(table, stride):
    for d in range(DAYS):
        table[d * stride : (d + 1) * stride, :] = jnp.zeros((stride, LANES), F32)


def add_up(bins, x, held, got, mean, total):
    stride = total + 1

    def add(t, carry):
        at = bins[t] * stride
        for k in range(total // 8):
            rows = pl.ds(at + 8 * k, 8)
            mean[rows, :] = mean[rows, :] + held[t, 8 * k : 8 * k + 8].astype(F32)
        return carry

    def adds(i, carry):
        enter(x, held, got, i).wait()
        return lax.fori_loop(0, SPAN, lambda t, c: add(i * SPAN + t, c), carry, unroll=4)

    lax.fori_loop(0, STEPS, adds, 0)


def enter(x, held, got, i):
    span = pl.ds(i * SPAN, SPAN)
    return pltpu.make_async_copy(x.at[span], held.at[span], got.at[i])


def divide(inverse, mean, packed, total):
    stride = total + 1
    for d in range(DAYS):
        rows = slice(d * stride, d * stride + total)
        value = mean[rows, :] * inverse[d]
        mean[rows, :] = value
        each = DAYS // len(packed)
        packed[d // each][d % each] = value.astype(BF16)


def powers(bins, held, mean, second, third, weight, norm, total, ready=None):
    stride = total + 1

    def one(t, carry):
        at = bins[t] * stride
        sums = None
        for k in range(total // 8):
            rows = pl.ds(at + 8 * k, 8)
            tile = slice(8 * k, 8 * k + 8)
            a = held[t, tile].astype(F32) - mean[rows, :]
            q = a * a
            second[rows, :] = second[rows, :] + q
            third[rows, :] = third[rows, :] + q * a
            w = q * weight[tile, :]
            sums = w if sums is None else sums + w
        norm[t] = sums
        return carry

    def some(i, carry):
        if ready is not None:
            ready(i)
        return lax.fori_loop(0, SPAN, lambda t, c: one(i * SPAN + t, c), carry, unroll=2 if total > 100 else 4)

    lax.fori_loop(0, STEPS, some, 0)


def total_norm(norm):
    return jnp.sum(jnp.sum(norm[...], axis=1).T, axis=0, keepdims=True)


def leave(wide, outs, put, first, count, i):
    return pltpu.make_async_copy(wide.at[i], outs[i].at[pl.ds(first, count)], put.at[i])


def sum_kernel(total, bins, inverse, x, mean, low, high, held, got):
    for i in range(STEPS):
        enter(x, held, got, i).start()
    zero(mean, total + 1)
    add_up(bins, x, held, got, mean, total)
    divide(inverse, mean, (low, high), total)


def table_shape(total):
    return (DAYS * (total + 1), LANES)


def half_shape(total):
    return jax.ShapeDtypeStruct((DAYS // 2, total, LANES), BF16)


def sums(bins, inverse, x, triples):
    total = rows_of(triples)
    return pl.pallas_call(
        functools.partial(sum_kernel, total),
        in_specs=[SMEM, SMEM, ANY],
        out_specs=[VMEM] * 3,
        out_shape=[jax.ShapeDtypeStruct(table_shape(total), F32), half_shape(total), half_shape(total)],
        scratch_shapes=[pltpu.VMEM((TIME, total, LANES), BF16), pltpu.SemaphoreType.DMA((STEPS,))],
        cost_estimate=pl.CostEstimate(flops=10_000_000 * triples, bytes_accessed=700_000 * triples, transcendentals=0),
        name="sums",
    )(bins, inverse, x)


def power_kernel(first, triples, bins, x, mean, scale, weight, *refs):
    outs, (after, held, second, third, norm, wide, got, put, _) = refs[:3], refs[3:]
    total = rows_of(triples)
    count = 3 * triples
    for i in range(STEPS):
        enter(x, held, got, i).start()
    zero(second, total + 1)
    zero(third, total + 1)
    unpack(mean, None, wide.at[0], triples)
    leave(wide, outs, put, first, count, 0).start()
    powers(
        bins, held, mean, second, third, weight, norm, total, lambda i: enter(x, held, got, i).wait()
    )
    after[...] = total_norm(norm)
    for i, table in ((1, second), (2, third)):
        unpack(table, scale[...], wide.at[i], triples)
        leave(wide, outs, put, first, count, i).start()
    for i in range(3):
        leave(wide, outs, put, first, count, i).wait()


FIELD = jax.ShapeDtypeStruct((BAND, DAYS, LAT), BF16)


def higher(bins, x, mean, scale, weight, first, triples):
    total = rows_of(triples)
    result = pl.pallas_call(
        functools.partial(power_kernel, first, triples),
        in_specs=[SMEM, ANY] + [VMEM] * 3,
        out_specs=[ANY] * 3 + [VMEM],
        out_shape=[FIELD] * 3 + [jax.ShapeDtypeStruct((1, TIME), F32)],
        scratch_shapes=[
            pltpu.VMEM((TIME, total, LANES), BF16),
            pltpu.VMEM(table_shape(total), F32),
            pltpu.VMEM(table_shape(total), F32),
            pltpu.VMEM((TIME, 8, LANES), F32),
            pltpu.VMEM((3, 3 * triples, DAYS, LAT), BF16),
            pltpu.SemaphoreType.DMA((STEPS,)),
            pltpu.SemaphoreType.DMA((3,)),
            pltpu.VMEM((SPARE, LANES), F32),
        ],
        cost_estimate=pl.CostEstimate(flops=40_000_000 * triples, bytes_accessed=1_000_000 * triples, transcendentals=0),
        name="higher",
    )(bins, x, mean, scale, weight)
    return result[:3], result[3]


def both_kernel(total, bins, inverse, x, weight, before, mean, second, third, packed, after, held, norm, got):
    for i in range(STEPS):
        enter(x, held, got, i).start()
    for table in (mean, second, third):
        zero(table, total + 1)
    add_up(bins, x, held, got, mean, total)
    divide(inverse, mean, (packed,), total)
    powers(bins, held, mean, second, third, weight, norm, total)
    row = before[...] + total_norm(norm)
    after[:, 0, :] = jnp.broadcast_to(row, (MODELS * PEERS, TIME))


def both(bins, inverse, x, weight, before, triples):
    total = rows_of(triples)
    table = jax.ShapeDtypeStruct(table_shape(total), F32)
    result = pl.pallas_call(
        functools.partial(both_kernel, total),
        in_specs=[SMEM, SMEM, ANY, VMEM, VMEM],
        out_specs=[VMEM] * 5,
        out_shape=[table] * 3
        + [jax.ShapeDtypeStruct((DAYS, total, LANES), BF16)]
        + [jax.ShapeDtypeStruct((MODELS * PEERS, 1, TIME), F32)],
        scratch_shapes=[
            pltpu.VMEM((TIME, total, LANES), BF16),
            pltpu.VMEM((TIME, 8, LANES), F32),
            pltpu.SemaphoreType.DMA((STEPS,)),
        ],
        cost_estimate=pl.CostEstimate(flops=50_000_000 * triples, bytes_accessed=1_000_000 * triples, transcendentals=0),
        name="both",
    )(bins, inverse, x, weight, before)
    return result[:3], result[3], result[4]


def unpack_kernel(first, triples, scale, *refs):
    tables, outs, wide, put = refs[:3], refs[6:9], refs[9], refs[10]
    for i in range(3):
        unpack(tables[i], None if i == 0 else scale[...], wide.at[i], triples)
        leave(wide, outs, put, first, 3 * triples, i).start()
    for i in range(3):
        leave(wide, outs, put, first, 3 * triples, i).wait()


def unpacked(scale, tables, outs, first, triples):
    return pl.pallas_call(
        functools.partial(unpack_kernel, first, triples),
        in_specs=[VMEM] * 4 + [ANY] * 3,
        out_specs=[ANY] * 3,
        out_shape=[FIELD] * 3,
        input_output_aliases={4: 0, 5: 1, 6: 2},
        scratch_shapes=[pltpu.VMEM((3, 3 * triples, DAYS, LAT), BF16), pltpu.SemaphoreType.DMA((3,))],
        cost_estimate=pl.CostEstimate(flops=3_000_000 * triples, bytes_accessed=700_000 * triples, transcendentals=0),
        name="unpacked",
    )(scale, *tables, *outs)


def family_kernel(first, triples, chained, pieces, share, *refs):
    means, refs = refs[: pieces * MODELS], refs[pieces * MODELS + (1 if chained else 0) :]
    each = DAYS // pieces
    out, table, wide, sem = refs
    total = rows_of(triples)
    stride = total + 1
    count = 3 * triples
    for d in range(DAYS):
        values = [means[pieces * k + d // each][d % each].astype(F32) for k in range(MODELS)]
        for f in range(FAM):
            value = values[0] * share[f, 0]
            for k in range(1, MODELS):
                value = value + values[k] * share[f, k]
            table[f, d * stride : d * stride + total, :] = value
    copies = []
    for f in range(FAM):
        unpack(table.at[f], None, wide.at[f], triples)
        copies.append(pltpu.make_async_copy(wide.at[f], out.at[f, pl.ds(first, count)], sem.at[f]))
        copies[-1].start()
    for copy in copies:
        copy.wait()


def families(share, means, out, first, triples):
    total = rows_of(triples)
    chained = out is not None
    return pl.pallas_call(
        functools.partial(family_kernel, first, triples, chained, len(means) // MODELS),
        in_specs=[SMEM] + [VMEM] * len(means) + [ANY] * (1 if chained else 0),
        out_specs=ANY,
        out_shape=jax.ShapeDtypeStruct((FAM, BAND, DAYS, LAT), BF16),
        input_output_aliases={1 + len(means): 0} if chained else {},
        scratch_shapes=[
            pltpu.VMEM((FAM, *table_shape(total)), F32),
            pltpu.VMEM((FAM, 3 * triples, DAYS, LAT), BF16),
            pltpu.SemaphoreType.DMA((FAM,)),
        ],
        cost_estimate=pl.CostEstimate(flops=10_000_000 * triples, bytes_accessed=500_000 * triples, transcendentals=0),
    )(share, *means, *(() if out is None else (out,)))


def moved(array, by):
    return lax.ppermute(array, "group", [(i, (i + by) % MODELS) for i in range(MODELS)])


def forwarded(low, high):
    behind_low = moved(low, 1)
    ahead_high = moved(high, -1)
    behind_high = moved(high, 1)
    ahead_low = moved(low, -1)
    across_low = moved(behind_low, 1)
    across_high = moved(ahead_high, -1)
    return [low, high, behind_low, behind_high, ahead_low, ahead_high, across_low, across_high]


def exchange(array):
    return lax.all_to_all(array, "tm", split_axis=0, concat_axis=0, tiled=True)


def local(precip, day_bins, family_of):
    sent = pack(precip[0])
    got0, later, day_bins, family_of = lax.optimization_barrier((exchange(sent[0]), sent[1], day_bins, family_of))
    got1 = exchange(later)

    days = jnp.arange(DAYS, dtype=jnp.int32)
    counts = jnp.sum((day_bins[None, :] == days[:, None]).astype(F32), axis=1)
    inverse = 1.0 / jnp.maximum(counts, 1.0)
    scale = jnp.broadcast_to(inverse[:, None], (DAYS, LANES))

    group = lax.axis_index("group")
    turned = (group + jnp.array([0, MODELS - 1, 1, 2], dtype=jnp.int32)) % MODELS
    models = jnp.arange(MODELS, dtype=jnp.int32)
    hot = (family_of[None, :] == jnp.arange(FAM, dtype=jnp.int32)[:, None]).astype(F32)
    members = jnp.maximum(jnp.sum(hot, axis=1), 1.0)
    at = (turned[:, None] == models[None, :]).astype(F32)
    share = jnp.sum(hot[:, None, :] * at[None], axis=2) / members[:, None]

    weight0, total_weight = packed_weight(CHUNKS[0])
    weight1, _ = packed_weight(CHUNKS[1])
    x0 = got0.reshape(TIME, rows_of(CHUNKS[0]), LANES)
    table0, low0, high0 = sums(day_bins, inverse, x0, CHUNKS[0])
    means0 = forwarded(low0, high0)
    outs, norm0 = higher(day_bins, x0, table0, scale, jnp.asarray(weight0), STARTS[0], CHUNKS[0])
    got1, norm0 = lax.optimization_barrier((got1, norm0))
    x1 = got1.reshape(TIME, rows_of(CHUNKS[1]), LANES)
    tables1, mean1, norm = both(day_bins, inverse, x1, jnp.asarray(weight1), norm0, CHUNKS[1])
    means1 = [mean1, *(moved(mean1, by) for by in (1, -1, 2))]
    parts = lax.all_to_all(norm, ("group", "tm"), split_axis=0, concat_axis=0, tiled=True)
    outs = unpacked(scale, tables1, outs, STARTS[1], CHUNKS[1])
    fam = families(share, means0, None, STARTS[0], CHUNKS[0])
    fam = families(share, means1, fam, STARTS[1], CHUNKS[1])

    anomaly_norm = jnp.sqrt(jnp.sum(parts.reshape(MODELS, PEERS, TIME), axis=1) / total_weight)
    fields = [o[None].transpose(0, 2, 1, 3) for o in outs]
    return (*fields, fam.transpose(0, 2, 1, 3), anomaly_norm)


def solution(mesh):
    in_specs = (P("group", "tm", None, None), P(), P())
    out_specs = (
        P("group", None, "tm", None),
        P("group", None, "tm", None),
        P("group", None, "tm", None),
        P(None, None, "tm", None),
        P(),
    )
    return jax.shard_map(local, mesh=mesh, in_specs=in_specs, out_specs=out_specs, check_vma=False)
```

```python
import functools
import math

import jax
import jax.numpy as jnp
import numpy as np
from jax import lax
from jax.experimental import pallas as pl
from jax.experimental.pallas import tpu as pltpu
from jax.sharding import PartitionSpec as P


LON = 1440
LAT = 720
DAYS = 16
FAM = 3
MODELS = 4
TIME = 128
LANES = 128
FULL = LAT // LANES
TAIL = LAT - FULL * LANES
HALF = TAIL // 2
PEERS = 32
BAND = LON // PEERS
BLOCK = 8 * BAND
CHUNKS = (11, 4)
STARTS = tuple(3 * sum(CHUNKS[:c]) for c in range(len(CHUNKS)))

SMEM = pl.BlockSpec(memory_space=pltpu.SMEM)
VMEM = pl.BlockSpec(memory_space=pltpu.VMEM)
ANY = pl.BlockSpec(memory_space=pl.ANY)
STEPS = 8
SPAN = TIME // STEPS

F32 = jnp.float32
BF16 = jnp.bfloat16


def rows_of(triples):
    return -(-17 * triples // 8) * 8


def packed_weight(triples):
    lat = np.arange(LAT, dtype=np.float64)
    weight = np.cos((-90.0 + (lat + 0.5) * 180.0 / LAT) * (math.pi / 180.0))
    count = 3 * triples
    rows = np.zeros((rows_of(triples), LANES))
    for j in range(FULL):
        rows[j * count : (j + 1) * count] = weight[j * LANES : (j + 1) * LANES]
    tail = weight[FULL * LANES :]
    for half in range(2):
        part = rows[FULL * count + half * triples : FULL * count + (half + 1) * triples]
        part[:, :TAIL] = tail
        part[:, TAIL : TAIL + HALF] = tail[half * HALF : (half + 1) * HALF]
    return rows.astype(np.float32), float(weight.sum() * LON)


def grant(mebibytes):
    return pltpu.CompilerParams(vmem_limit_bytes=mebibytes * 2**20)


def pack_rows(first, triples, wide, rows, ready):
    count = 3 * triples
    lane = lax.broadcasted_iota(jnp.int32, (triples, LANES), 1)
    for r in range(8):
        s = BAND * r + first
        for j in range(FULL):
            rows[j * count : (j + 1) * count, :] = wide[j, s : s + count, :]
        third = wide[FULL, s + 2 * triples : s + 3 * triples, :]
        for half in range(2):
            own = wide[FULL, s + half * triples : s + (half + 1) * triples, :]
            moved = pltpu.roll(third, TAIL - half * HALF, 1)
            rows[FULL * count + half * triples : FULL * count + (half + 1) * triples, :] = jnp.where(
                lane < TAIL, own, jnp.where(lane < TAIL + HALF, moved, 0.0)
            )
        ready[r] = rows[...].astype(BF16)


def pack_kernel(steps, x, *refs):
    n = len(CHUNKS)
    outs, held, ready, wide = refs[:n], refs[n], refs[n + 1 : 2 * n + 1], refs[2 * n + 1]
    rows, got, put = refs[2 * n + 2 : 3 * n + 2], refs[3 * n + 2], refs[3 * n + 3]
    pieces = LON // BLOCK * steps

    def enter(i):
        q, t = i // steps, i % steps
        return pltpu.make_async_copy(x.at[t, pl.ds(pl.multiple_of(q * BLOCK, 8), BLOCK)], held.at[i], got.at[i])

    def leave(c, i):
        q, t = i // steps, i % steps
        return pltpu.make_async_copy(ready[c].at[i], outs[c].at[pl.ds(q * 8, 8), t], put.at[c, i])

    for i in range(pieces):
        enter(i).start()
    for c, triples in enumerate(CHUNKS):
        total = rows_of(triples)
        rows[c][total - 8 :, :] = jnp.zeros((8, LANES), F32)

    def piece(i, carry):
        enter(i).wait()
        for j in range(FULL):
            wide[j] = held[i, :, j * LANES : (j + 1) * LANES].astype(F32)
        wide[FULL, :, :TAIL] = held[i, :, FULL * LANES :].astype(F32)
        for c, triples in enumerate(CHUNKS):
            pack_rows(STARTS[c], triples, wide, rows[c], ready[c].at[i])
            leave(c, i).start()
        return carry

    lax.fori_loop(0, pieces, piece, 0)
    for c in range(n):
        for i in range(pieces):
            leave(c, i).wait()


def pack(x):
    steps = x.shape[0]
    totals = [rows_of(n) for n in CHUNKS]
    pieces = LON // BLOCK * steps
    return pl.pallas_call(
        functools.partial(pack_kernel, steps),
        in_specs=[ANY],
        out_specs=[ANY] * len(CHUNKS),
        out_shape=[jax.ShapeDtypeStruct((PEERS, steps, total, LANES), BF16) for total in totals],
        scratch_shapes=[pltpu.VMEM((pieces, BLOCK, LAT), BF16)]
        + [pltpu.VMEM((pieces, 8, total, LANES), BF16) for total in totals]
        + [pltpu.VMEM((FULL + 1, BLOCK, LANES), F32)]
        + [pltpu.VMEM((total, LANES), F32) for total in totals]
        + [pltpu.SemaphoreType.DMA((pieces,)), pltpu.SemaphoreType.DMA((len(CHUNKS), pieces))],
        cost_estimate=pl.CostEstimate(flops=10_000_000, bytes_accessed=17_000_000, transcendentals=0),
        name="pack",
    )(x)


def day_rows(table, stride, index):
    halves = [table[pl.ds(8 * h * stride + index, 8, stride=stride), :] for h in range(DAYS // 8)]
    return jnp.concatenate(halves, axis=0)


def unpack_rows(row, outs, triples):
    count = 3 * triples
    lane = lax.broadcasted_iota(jnp.int32, (DAYS, LANES), 1)

    def whole(lon, carry):
        for j in range(FULL):
            for out, value in zip(outs, row(j * count + lon)):
                out[lon, :, j * LANES : (j + 1) * LANES] = value.astype(BF16)
        return carry

    def tail(lon, carry):
        for out, value in zip(outs, row(FULL * count + lon)):
            out[lon, :, FULL * LANES :] = value[:, :TAIL].astype(BF16)
        return carry

    def last(k, carry):
        for out, low, high in zip(outs, row(FULL * count + k), row(FULL * count + triples + k)):
            low = pltpu.roll(low, LANES - TAIL, 1)
            high = pltpu.roll(high, LANES - TAIL + HALF, 1)
            joined = jnp.where(lane < HALF, low, high)
            out[2 * triples + k, :, FULL * LANES :] = joined[:, :TAIL].astype(BF16)
        return carry

    lax.fori_loop(0, count, whole, 0, unroll=3)
    lax.fori_loop(0, 2 * triples, tail, 0, unroll=2)
    lax.fori_loop(0, triples, last, 0)


def unpack(table, scale, out, triples):
    stride = rows_of(triples) + 1

    def row(index):
        value = day_rows(table, stride, index)
        return [value if scale is None else value * scale]

    unpack_rows(row, [out], triples)


def zero(table, stride):
    for d in range(DAYS):
        table[d * stride : (d + 1) * stride, :] = jnp.zeros((stride, LANES), F32)


def add_up(bins, x, held, got, mean, total):
    stride = total + 1

    def add(t, carry):
        at = bins[t] * stride
        for k in range(total // 8):
            rows = pl.ds(at + 8 * k, 8)
            mean[rows, :] = mean[rows, :] + held[t, 8 * k : 8 * k + 8].astype(F32)
        return carry

    def adds(i, carry):
        enter(x, held, got, i).wait()
        return lax.fori_loop(0, SPAN, lambda t, c: add(i * SPAN + t, c), carry, unroll=4)

    lax.fori_loop(0, STEPS, adds, 0)


def enter(x, held, got, i):
    span = pl.ds(i * SPAN, SPAN)
    return pltpu.make_async_copy(x.at[span], held.at[span], got.at[i])


def divide(inverse, scale, mean, packed, total):
    stride = total + 1
    each = total // len(packed)

    def one(k, carry):
        for p, rows in enumerate(packed):
            rows[k] = (day_rows(mean, stride, p * each + k) * scale[...]).astype(BF16)
        return carry

    lax.fori_loop(0, each, one, 0, unroll=4)
    for d in range(DAYS):
        rows = slice(d * stride, d * stride + total)
        mean[rows, :] = mean[rows, :] * inverse[d]


def powers(bins, held, mean, second, third, weight, norm, total, ready=None):
    stride = total + 1

    def one(t, carry):
        at = bins[t] * stride
        sums = None
        for k in range(total // 8):
            rows = pl.ds(at + 8 * k, 8)
            tile = slice(8 * k, 8 * k + 8)
            a = held[t, tile].astype(F32) - mean[rows, :]
            q = a * a
            second[rows, :] = second[rows, :] + q
            third[rows, :] = third[rows, :] + q * a
            w = q * weight[tile, :]
            sums = w if sums is None else sums + w
        norm[t] = sums
        return carry

    def some(i, carry):
        if ready is not None:
            ready(i)
        return lax.fori_loop(0, SPAN, lambda t, c: one(i * SPAN + t, c), carry, unroll=2 if total > 100 else 4)

    lax.fori_loop(0, STEPS, some, 0)


def total_norm(norm):
    return jnp.sum(jnp.sum(norm[...], axis=1).T, axis=0, keepdims=True)


def leave(wide, outs, put, first, count, i):
    return pltpu.make_async_copy(wide.at[i], outs[i].at[pl.ds(first, count)], put.at[i])


def sum_kernel(total, bins, inverse, scale, x, mean, low, high, held, got):
    for i in range(STEPS):
        enter(x, held, got, i).start()
    zero(mean, total + 1)
    add_up(bins, x, held, got, mean, total)
    divide(inverse, scale, mean, (low, high), total)


def table_shape(total):
    return (DAYS * (total + 1), LANES)


def row_shape(total):
    return jax.ShapeDtypeStruct((total, DAYS, LANES), BF16)


def sums(bins, inverse, scale, x, triples):
    total = rows_of(triples)
    return pl.pallas_call(
        functools.partial(sum_kernel, total),
        in_specs=[SMEM, SMEM, VMEM, ANY],
        out_specs=[VMEM] * 3,
        out_shape=[jax.ShapeDtypeStruct(table_shape(total), F32)] + [row_shape(total // 2)] * 2,
        scratch_shapes=[pltpu.VMEM((TIME, total, LANES), BF16), pltpu.SemaphoreType.DMA((STEPS,))],
        cost_estimate=pl.CostEstimate(flops=10_000_000 * triples, bytes_accessed=700_000 * triples, transcendentals=0),
        name="sums",
    )(bins, inverse, scale, x)


def power_kernel(first, triples, bins, x, mean, scale, weight, *refs):
    outs, (after, held, second, third, norm, wide, got, put) = refs[:3], refs[3:]
    total = rows_of(triples)
    count = 3 * triples
    for i in range(STEPS):
        enter(x, held, got, i).start()
    zero(second, total + 1)
    zero(third, total + 1)
    unpack(mean, None, wide.at[0], triples)
    leave(wide, outs, put, first, count, 0).start()
    powers(
        bins, held, mean, second, third, weight, norm, total, lambda i: enter(x, held, got, i).wait()
    )
    after[...] = total_norm(norm)
    for i, table in ((1, second), (2, third)):
        unpack(table, scale[...], wide.at[i], triples)
        leave(wide, outs, put, first, count, i).start()
    for i in range(3):
        leave(wide, outs, put, first, count, i).wait()


FIELD = jax.ShapeDtypeStruct((BAND, DAYS, LAT), BF16)


def higher(bins, x, mean, scale, weight, first, triples):
    total = rows_of(triples)
    result = pl.pallas_call(
        functools.partial(power_kernel, first, triples),
        in_specs=[SMEM, ANY] + [VMEM] * 3,
        out_specs=[ANY] * 3 + [VMEM],
        out_shape=[FIELD] * 3 + [jax.ShapeDtypeStruct((1, TIME), F32)],
        scratch_shapes=[
            pltpu.VMEM((TIME, total, LANES), BF16),
            pltpu.VMEM(table_shape(total), F32),
            pltpu.VMEM(table_shape(total), F32),
            pltpu.VMEM((TIME, 8, LANES), F32),
            pltpu.VMEM((3, 3 * triples, DAYS, LAT), BF16),
            pltpu.SemaphoreType.DMA((STEPS,)),
            pltpu.SemaphoreType.DMA((3,)),
        ],
        cost_estimate=pl.CostEstimate(flops=40_000_000 * triples, bytes_accessed=1_000_000 * triples, transcendentals=0),
        name="higher",
    )(bins, x, mean, scale, weight)
    return result[:3], result[3]


def both_kernel(first, triples, bins, inverse, scale, x, weight, before, *refs):
    outs, (packed, after, held, mean, second, third, norm, wide, got, put) = refs[3:6], refs[6:]
    total = rows_of(triples)
    count = 3 * triples
    for i in range(STEPS):
        enter(x, held, got, i).start()
    for table in (mean, second, third):
        zero(table, total + 1)
    add_up(bins, x, held, got, mean, total)
    divide(inverse, scale, mean, (packed,), total)
    unpack(mean, None, wide.at[0], triples)
    leave(wide, outs, put, first, count, 0).start()
    powers(bins, held, mean, second, third, weight, norm, total)
    row = before[...] + total_norm(norm)
    after[:, 0, :] = jnp.broadcast_to(row, (MODELS * PEERS, TIME))
    for i, table in ((1, second), (2, third)):
        unpack(table, scale[...], wide.at[i], triples)
        leave(wide, outs, put, first, count, i).start()
    for i in range(3):
        leave(wide, outs, put, first, count, i).wait()


def both(bins, inverse, scale, x, weight, before, outs, first, triples):
    total = rows_of(triples)
    result = pl.pallas_call(
        functools.partial(both_kernel, first, triples),
        in_specs=[SMEM, SMEM, VMEM, ANY, VMEM, VMEM] + [ANY] * 3,
        out_specs=[ANY] * 3 + [VMEM] * 2,
        out_shape=[FIELD] * 3 + [row_shape(total), jax.ShapeDtypeStruct((MODELS * PEERS, 1, TIME), F32)],
        input_output_aliases={6: 0, 7: 1, 8: 2},
        scratch_shapes=[
            pltpu.VMEM((TIME, total, LANES), BF16),
            pltpu.VMEM(table_shape(total), F32),
            pltpu.VMEM(table_shape(total), F32),
            pltpu.VMEM(table_shape(total), F32),
            pltpu.VMEM((TIME, 8, LANES), F32),
            pltpu.VMEM((3, 3 * triples, DAYS, LAT), BF16),
            pltpu.SemaphoreType.DMA((STEPS,)),
            pltpu.SemaphoreType.DMA((3,)),
        ],
        cost_estimate=pl.CostEstimate(flops=50_000_000 * triples, bytes_accessed=1_000_000 * triples, transcendentals=0),
        name="both",
        compiler_params=grant(24),
    )(bins, inverse, scale, x, weight, before, *outs)
    return result[:3], result[3], result[4]


def family_kernel(first, triples, chained, pieces, share, *refs):
    means, refs = refs[: pieces * MODELS], refs[pieces * MODELS + (1 if chained else 0) :]
    out, held, wide, got, put = refs
    total = rows_of(triples)
    count = 3 * triples
    each = total // pieces

    def enter(i):
        k, p = i // pieces, i % pieces
        return pltpu.make_async_copy(means[i], held.at[k, pl.ds(p * each, each)], got.at[i])

    def leave(f):
        return pltpu.make_async_copy(wide.at[f], out.at[f, pl.ds(first, count)], put.at[f])

    for i in range(pieces * MODELS):
        enter(i).start()
    for i in range(pieces * MODELS):
        enter(i).wait()
    shares = [[share[f, k] for k in range(MODELS)] for f in range(FAM)]

    def row(index):
        values = [held[k, index].astype(F32) for k in range(MODELS)]
        results = []
        for f in range(FAM):
            value = values[0] * shares[f][0]
            for k in range(1, MODELS):
                value = value + values[k] * shares[f][k]
            results.append(value)
        return results

    unpack_rows(row, [wide.at[f] for f in range(FAM)], triples)
    for f in range(FAM):
        leave(f).start()
    for f in range(FAM):
        leave(f).wait()


def families(share, means, out, first, triples):
    total = rows_of(triples)
    chained = out is not None
    return pl.pallas_call(
        functools.partial(family_kernel, first, triples, chained, len(means) // MODELS),
        in_specs=[SMEM] + [ANY] * len(means) + [ANY] * (1 if chained else 0),
        out_specs=ANY,
        out_shape=jax.ShapeDtypeStruct((FAM, BAND, DAYS, LAT), BF16),
        input_output_aliases={1 + len(means): 0} if chained else {},
        scratch_shapes=[
            pltpu.VMEM((MODELS, total, DAYS, LANES), BF16),
            pltpu.VMEM((FAM, 3 * triples, DAYS, LAT), BF16),
            pltpu.SemaphoreType.DMA((len(means),)),
            pltpu.SemaphoreType.DMA((FAM,)),
        ],
        cost_estimate=pl.CostEstimate(flops=10_000_000 * triples, bytes_accessed=500_000 * triples, transcendentals=0),
        compiler_params=grant(12) if chained else None,
    )(share, *means, *(() if out is None else (out,)))


def moved(array, by):
    return lax.ppermute(array, "group", [(i, (i + by) % MODELS) for i in range(MODELS)])


def forwarded(low, high):
    behind_low = moved(low, 1)
    ahead_high = moved(high, -1)
    behind_high = moved(high, 1)
    ahead_low = moved(low, -1)
    across_low = moved(behind_low, 1)
    across_high = moved(ahead_high, -1)
    return [low, high, behind_low, behind_high, ahead_low, ahead_high, across_low, across_high]


def exchange(array):
    return lax.all_to_all(array, "tm", split_axis=0, concat_axis=0, tiled=True)


def local(precip, day_bins, family_of):
    sent = pack(precip[0])
    got0, later, day_bins, family_of = lax.optimization_barrier((exchange(sent[0]), sent[1], day_bins, family_of))
    got1 = exchange(later)

    days = jnp.arange(DAYS, dtype=jnp.int32)
    counts = jnp.sum((day_bins[None, :] == days[:, None]).astype(F32), axis=1)
    inverse = 1.0 / jnp.maximum(counts, 1.0)
    scale = jnp.broadcast_to(inverse[:, None], (DAYS, LANES))

    group = lax.axis_index("group")
    turned = (group + jnp.array([0, MODELS - 1, 1, 2], dtype=jnp.int32)) % MODELS
    models = jnp.arange(MODELS, dtype=jnp.int32)
    hot = (family_of[None, :] == jnp.arange(FAM, dtype=jnp.int32)[:, None]).astype(F32)
    members = jnp.maximum(jnp.sum(hot, axis=1), 1.0)
    at = (turned[:, None] == models[None, :]).astype(F32)
    share = jnp.sum(hot[:, None, :] * at[None], axis=2) / members[:, None]

    weight0, total_weight = packed_weight(CHUNKS[0])
    weight1, _ = packed_weight(CHUNKS[1])
    x0 = got0.reshape(TIME, rows_of(CHUNKS[0]), LANES)
    table0, low0, high0 = sums(day_bins, inverse, scale, x0, CHUNKS[0])
    means0 = forwarded(low0, high0)
    outs, norm0 = higher(day_bins, x0, table0, scale, jnp.asarray(weight0), STARTS[0], CHUNKS[0])
    got1, norm0 = lax.optimization_barrier((got1, norm0))
    x1 = got1.reshape(TIME, rows_of(CHUNKS[1]), LANES)
    outs, mean1, norm = both(
        day_bins, inverse, scale, x1, jnp.asarray(weight1), norm0, outs, STARTS[1], CHUNKS[1]
    )
    means1 = [mean1, *(moved(mean1, by) for by in (1, -1, 2))]
    parts = lax.all_to_all(norm, ("group", "tm"), split_axis=0, concat_axis=0, tiled=True)
    fam = families(share, means0, None, STARTS[0], CHUNKS[0])
    fam = families(share, means1, fam, STARTS[1], CHUNKS[1])

    anomaly_norm = jnp.sqrt(jnp.sum(parts.reshape(MODELS, PEERS, TIME), axis=1) / total_weight)
    fields = [o[None].transpose(0, 2, 1, 3) for o in outs]
    return (*fields, fam.transpose(0, 2, 1, 3), anomaly_norm)


def solution(mesh):
    in_specs = (P("group", "tm", None, None), P(), P())
    out_specs = (
        P("group", None, "tm", None),
        P("group", None, "tm", None),
        P("group", None, "tm", None),
        P(None, None, "tm", None),
        P(),
    )
    return jax.shard_map(local, mesh=mesh, in_specs=in_specs, out_specs=out_specs, check_vma=False)
```

```python
import functools
import math

import jax
import jax.numpy as jnp
import numpy as np
from jax import lax
from jax.experimental import pallas as pl
from jax.experimental.pallas import tpu as pltpu
from jax.sharding import PartitionSpec as P


LON = 1440
LAT = 720
DAYS = 16
FAM = 3
MODELS = 4
TIME = 128
LANES = 128
FULL = LAT // LANES
TAIL = LAT - FULL * LANES
HALF = TAIL // 2
PEERS = 32
BAND = LON // PEERS
BLOCK = 8 * BAND
CHUNKS = ((15, 16), (14,))
STARTS = tuple(sum(map(sum, CHUNKS[:c])) for c in range(len(CHUNKS)))

SMEM = pl.BlockSpec(memory_space=pltpu.SMEM)
VMEM = pl.BlockSpec(memory_space=pltpu.VMEM)
ANY = pl.BlockSpec(memory_space=pl.ANY)
STEPS = 8
LIMITS = (None, None, 12)
SPAN = TIME // STEPS

F32 = jnp.float32
BF16 = jnp.bfloat16


def tails_of(count):
    return -(-2 * count // 3)


def block_rows(count):
    return FULL * count + tails_of(count)


def rows_of(chunk):
    return -(-sum(map(block_rows, chunk)) // 8) * 8


def blocks_of(chunk):
    lon = row = 0
    for count in chunk:
        yield lon, row, count, tails_of(count), count - tails_of(count)
        lon += count
        row += block_rows(count)


def packed_weight(chunk):
    lat = np.arange(LAT, dtype=np.float64)
    weight = np.cos((-90.0 + (lat + 0.5) * 180.0 / LAT) * (math.pi / 180.0))
    rows = np.zeros((rows_of(chunk), LANES))
    left = weight[FULL * LANES :]
    for _, base, count, tails, split in blocks_of(chunk):
        for j in range(FULL):
            rows[base + j * count : base + (j + 1) * count] = weight[j * LANES : (j + 1) * LANES]
        at = base + FULL * count
        rows[at : at + tails, :TAIL] = left
        for half in range(2):
            part = rows[at + half * split : at + (half + 1) * split]
            part[:, TAIL : TAIL + HALF] = left[half * HALF : (half + 1) * HALF]
    return rows.astype(np.float32), float(weight.sum() * LON)


def loop(length, body, unroll):
    def some(k, carry):
        for i in range(unroll):
            body(k * unroll + i)
        return carry

    lax.fori_loop(0, length // unroll, some, 0)
    for i in range(length - length % unroll, length):
        body(i)


def grant(mebibytes):
    return pltpu.CompilerParams(vmem_limit_bytes=mebibytes * 2**20)


def pack_rows(first, chunk, wide, rows, ready):
    for r in range(8):
        for lon, base, count, tails, split in blocks_of(chunk):
            s = BAND * r + first + lon
            for j in range(FULL):
                rows[base + j * count : base + (j + 1) * count, :] = wide[j, s : s + count, :]
            at = base + FULL * count
            lane = lax.broadcasted_iota(jnp.int32, (split, LANES), 1)
            third = wide[FULL, s + tails : s + count, :]
            for half in range(2):
                own = wide[FULL, s + half * split : s + (half + 1) * split, :]
                moved = pltpu.roll(third, TAIL - half * HALF, 1)
                rows[at + half * split : at + (half + 1) * split, :] = jnp.where(
                    lane < TAIL, own, jnp.where(lane < TAIL + HALF, moved, 0.0)
                )
            if tails > 2 * split:
                own = wide[FULL, s + 2 * split : s + tails, :]
                lane = lax.broadcasted_iota(jnp.int32, own.shape, 1)
                rows[at + 2 * split : at + tails, :] = jnp.where(lane < TAIL, own, 0.0)
        ready[r] = rows[...].astype(BF16)


def pack_kernel(steps, x, *refs):
    n = len(CHUNKS)
    outs, held, ready, wide = refs[:n], refs[n], refs[n + 1 : 2 * n + 1], refs[2 * n + 1]
    rows, got, put = refs[2 * n + 2 : 3 * n + 2], refs[3 * n + 2], refs[3 * n + 3]
    pieces = LON // BLOCK * steps

    def enter(i):
        q, t = i // steps, i % steps
        return pltpu.make_async_copy(x.at[t, pl.ds(pl.multiple_of(q * BLOCK, 8), BLOCK)], held.at[i], got.at[i])

    def leave(c, i):
        q, t = i // steps, i % steps
        return pltpu.make_async_copy(ready[c].at[i], outs[c].at[pl.ds(q * 8, 8), t], put.at[c, i])

    for i in range(pieces):
        enter(i).start()
    for c, chunk in enumerate(CHUNKS):
        total = rows_of(chunk)
        rows[c][total - 8 :, :] = jnp.zeros((8, LANES), F32)

    def piece(i, carry):
        enter(i).wait()
        for j in range(FULL):
            wide[j] = held[i, :, j * LANES : (j + 1) * LANES].astype(F32)
        wide[FULL, :, :TAIL] = held[i, :, FULL * LANES :].astype(F32)
        for c, chunk in enumerate(CHUNKS):
            pack_rows(STARTS[c], chunk, wide, rows[c], ready[c].at[i])
            leave(c, i).start()
        return carry

    lax.fori_loop(0, pieces, piece, 0)
    for c in range(n):
        for i in range(pieces):
            leave(c, i).wait()


def pack(x):
    steps = x.shape[0]
    totals = [rows_of(n) for n in CHUNKS]
    pieces = LON // BLOCK * steps
    return pl.pallas_call(
        functools.partial(pack_kernel, steps),
        in_specs=[ANY],
        out_specs=[ANY] * len(CHUNKS),
        out_shape=[jax.ShapeDtypeStruct((PEERS, steps, total, LANES), BF16) for total in totals],
        scratch_shapes=[pltpu.VMEM((pieces, BLOCK, LAT), BF16)]
        + [pltpu.VMEM((pieces, 8, total, LANES), BF16) for total in totals]
        + [pltpu.VMEM((FULL + 1, BLOCK, LANES), F32)]
        + [pltpu.VMEM((total, LANES), F32) for total in totals]
        + [pltpu.SemaphoreType.DMA((pieces,)), pltpu.SemaphoreType.DMA((len(CHUNKS), pieces))],
        cost_estimate=pl.CostEstimate(flops=10_000_000, bytes_accessed=17_000_000, transcendentals=0),
        name="pack",
    )(x)


def day_rows(table, stride, index):
    halves = [table[pl.ds(8 * h * stride + index, 8, stride=stride), :] for h in range(DAYS // 8)]
    return jnp.concatenate(halves, axis=0)


def unpack_rows(row, outs, block):
    first, base, count, tails, split = block
    lane = lax.broadcasted_iota(jnp.int32, (DAYS, LANES), 1)
    at = base + FULL * count

    def whole(lon):
        for j in range(FULL):
            for out, value in zip(outs, row(base + j * count + lon)):
                out[first + lon, :, j * LANES : (j + 1) * LANES] = value.astype(BF16)

    def tail(lon):
        for out, value in zip(outs, row(at + lon)):
            out[first + lon, :, FULL * LANES :] = value[:, :TAIL].astype(BF16)

    def last(k):
        for out, low, high in zip(outs, row(at + k), row(at + split + k)):
            low = pltpu.roll(low, LANES - TAIL, 1)
            high = pltpu.roll(high, LANES - TAIL + HALF, 1)
            joined = jnp.where(lane < HALF, low, high)
            out[first + tails + k, :, FULL * LANES :] = joined[:, :TAIL].astype(BF16)

    loop(count, whole, 3)
    loop(tails, tail, 2)
    loop(split, last, 1)


def unpack(table, scale, out, chunk):
    stride = rows_of(chunk) + 1

    def row(index):
        value = day_rows(table, stride, index)
        return [value if scale is None else value * scale]

    for block in blocks_of(chunk):
        unpack_rows(row, [out], block)


def zero(table, stride):
    for d in range(DAYS):
        table[d * stride : (d + 1) * stride, :] = jnp.zeros((stride, LANES), F32)


def add_up(bins, x, held, got, mean, total):
    stride = total + 1

    def add(t, carry):
        at = bins[t] * stride
        for k in range(total // 8):
            rows = pl.ds(at + 8 * k, 8)
            mean[rows, :] = mean[rows, :] + held[t, 8 * k : 8 * k + 8].astype(F32)
        return carry

    def adds(i, carry):
        enter(x, held, got, i).wait()
        return lax.fori_loop(0, SPAN, lambda t, c: add(i * SPAN + t, c), carry, unroll=4)

    lax.fori_loop(0, STEPS, adds, 0)


def enter(x, held, got, i):
    span = pl.ds(i * SPAN, SPAN)
    return pltpu.make_async_copy(x.at[span], held.at[span], got.at[i])


def divide(inverse, scale, mean, packed, total):
    stride = total + 1
    base = 0
    for rows in packed:

        def one(k, rows=rows, base=base):
            rows[k] = (day_rows(mean, stride, base + k) * scale[...]).astype(BF16)

        loop(rows.shape[0], one, 4)
        base += rows.shape[0]
    for d in range(DAYS):
        rows = slice(d * stride, d * stride + total)
        mean[rows, :] = mean[rows, :] * inverse[d]


def powers(bins, held, mean, second, third, weight, norm, total, ready=None):
    stride = total + 1

    def one(t, carry):
        at = bins[t] * stride
        sums = None
        for k in range(total // 8):
            rows = pl.ds(at + 8 * k, 8)
            tile = slice(8 * k, 8 * k + 8)
            a = held[t, tile].astype(F32) - mean[rows, :]
            q = a * a
            second[rows, :] = second[rows, :] + q
            third[rows, :] = third[rows, :] + q * a
            w = q * weight[tile, :]
            sums = w if sums is None else sums + w
        norm[t] = sums
        return carry

    def some(i, carry):
        if ready is not None:
            ready(i)
        return lax.fori_loop(0, SPAN, lambda t, c: one(i * SPAN + t, c), carry, unroll=2 if total > 100 else 4)

    lax.fori_loop(0, STEPS, some, 0)


def total_norm(norm):
    return jnp.sum(jnp.sum(norm[...], axis=1).T, axis=0, keepdims=True)


def leave(wide, outs, put, first, count, i):
    return pltpu.make_async_copy(wide.at[i], outs[i].at[pl.ds(first, count)], put.at[i])


def sum_kernel(total, bins, inverse, scale, x, mean, *refs):
    packed, held, got = refs[:-2], refs[-2], refs[-1]
    for i in range(STEPS):
        enter(x, held, got, i).start()
    zero(mean, total + 1)
    add_up(bins, x, held, got, mean, total)
    divide(inverse, scale, mean, packed, total)


def table_shape(total):
    return (DAYS * (total + 1), LANES)


def row_shape(total):
    return jax.ShapeDtypeStruct((total, DAYS, LANES), BF16)


def sums(bins, inverse, scale, x, chunk):
    total = rows_of(chunk)
    return pl.pallas_call(
        functools.partial(sum_kernel, total),
        in_specs=[SMEM, SMEM, VMEM, ANY],
        out_specs=[VMEM] * (1 + len(chunk)),
        out_shape=[jax.ShapeDtypeStruct(table_shape(total), F32)] + [row_shape(block_rows(n)) for n in chunk],
        scratch_shapes=[pltpu.VMEM((TIME, total, LANES), BF16), pltpu.SemaphoreType.DMA((STEPS,))],
        cost_estimate=pl.CostEstimate(flops=3_000_000 * sum(chunk), bytes_accessed=230_000 * sum(chunk), transcendentals=0),
        name="sums",
    )(bins, inverse, scale, x)


def power_kernel(first, chunk, bins, x, mean, scale, weight, *refs):
    outs, (after, held, second, third, norm, wide, got, put) = refs[:3], refs[3:]
    total = rows_of(chunk)
    count = sum(chunk)
    for i in range(STEPS):
        enter(x, held, got, i).start()
    zero(second, total + 1)
    zero(third, total + 1)
    unpack(mean, None, wide.at[0], chunk)
    leave(wide, outs, put, first, count, 0).start()
    powers(
        bins, held, mean, second, third, weight, norm, total, lambda i: enter(x, held, got, i).wait()
    )
    after[...] = total_norm(norm)
    for i, table in ((1, second), (2, third)):
        unpack(table, scale[...], wide.at[i], chunk)
        leave(wide, outs, put, first, count, i).start()
    for i in range(3):
        leave(wide, outs, put, first, count, i).wait()


FIELD = jax.ShapeDtypeStruct((BAND, DAYS, LAT), BF16)


def higher(bins, x, mean, scale, weight, first, chunk):
    total = rows_of(chunk)
    result = pl.pallas_call(
        functools.partial(power_kernel, first, chunk),
        in_specs=[SMEM, ANY] + [VMEM] * 3,
        out_specs=[ANY] * 3 + [VMEM],
        out_shape=[FIELD] * 3 + [jax.ShapeDtypeStruct((1, TIME), F32)],
        scratch_shapes=[
            pltpu.VMEM((TIME, total, LANES), BF16),
            pltpu.VMEM(table_shape(total), F32),
            pltpu.VMEM(table_shape(total), F32),
            pltpu.VMEM((TIME, 8, LANES), F32),
            pltpu.VMEM((3, sum(chunk), DAYS, LAT), BF16),
            pltpu.SemaphoreType.DMA((STEPS,)),
            pltpu.SemaphoreType.DMA((3,)),
        ],
        cost_estimate=pl.CostEstimate(flops=13_000_000 * sum(chunk), bytes_accessed=330_000 * sum(chunk), transcendentals=0),
        name="higher",
    )(bins, x, mean, scale, weight)
    return result[:3], result[3]


def both_kernel(first, chunk, bins, inverse, scale, x, weight, before, *refs):
    outs, (packed, after, held, mean, second, third, norm, wide, got, put) = refs[3:6], refs[6:]
    total = rows_of(chunk)
    count = sum(chunk)
    for i in range(STEPS):
        enter(x, held, got, i).start()
    for table in (mean, second, third):
        zero(table, total + 1)
    add_up(bins, x, held, got, mean, total)
    divide(inverse, scale, mean, (packed,), total)
    unpack(mean, None, wide.at[0], chunk)
    leave(wide, outs, put, first, count, 0).start()
    powers(bins, held, mean, second, third, weight, norm, total)
    row = before[...] + total_norm(norm)
    after[:, 0, :] = jnp.broadcast_to(row, (MODELS * PEERS, TIME))
    for i, table in ((1, second), (2, third)):
        unpack(table, scale[...], wide.at[i], chunk)
        leave(wide, outs, put, first, count, i).start()
    for i in range(3):
        leave(wide, outs, put, first, count, i).wait()


def both(bins, inverse, scale, x, weight, before, outs, first, chunk):
    total = rows_of(chunk)
    result = pl.pallas_call(
        functools.partial(both_kernel, first, chunk),
        in_specs=[SMEM, SMEM, VMEM, ANY, VMEM, VMEM] + [ANY] * 3,
        out_specs=[ANY] * 3 + [VMEM] * 2,
        out_shape=[FIELD] * 3 + [row_shape(block_rows(*chunk)), jax.ShapeDtypeStruct((MODELS * PEERS, 1, TIME), F32)],
        input_output_aliases={6: 0, 7: 1, 8: 2},
        scratch_shapes=[
            pltpu.VMEM((TIME, total, LANES), BF16),
            pltpu.VMEM(table_shape(total), F32),
            pltpu.VMEM(table_shape(total), F32),
            pltpu.VMEM(table_shape(total), F32),
            pltpu.VMEM((TIME, 8, LANES), F32),
            pltpu.VMEM((3, sum(chunk), DAYS, LAT), BF16),
            pltpu.SemaphoreType.DMA((STEPS,)),
            pltpu.SemaphoreType.DMA((3,)),
        ],
        cost_estimate=pl.CostEstimate(flops=16_000_000 * sum(chunk), bytes_accessed=330_000 * sum(chunk), transcendentals=0),
        name="both",
        compiler_params=grant(24),
    )(bins, inverse, scale, x, weight, before, *outs)
    return result[:3], result[3], result[4]


def family_kernel(first, count, chained, share, *refs):
    means = refs[:MODELS]
    out, held, wide, got, put = refs[MODELS + (1 if chained else 0) :]

    def enter(k):
        return pltpu.make_async_copy(means[k], held.at[k], got.at[k])

    def leave(f):
        return pltpu.make_async_copy(wide.at[f], out.at[f, pl.ds(first, count)], put.at[f])

    for k in range(MODELS):
        enter(k).start()
    for k in range(MODELS):
        enter(k).wait()
    shares = [[share[f, k] for k in range(MODELS)] for f in range(FAM)]

    def row(index):
        values = [held[k, index].astype(F32) for k in range(MODELS)]
        results = []
        for f in range(FAM):
            value = values[0] * shares[f][0]
            for k in range(1, MODELS):
                value = value + values[k] * shares[f][k]
            results.append(value)
        return results

    (block,) = blocks_of((count,))
    unpack_rows(row, [wide.at[f] for f in range(FAM)], block)
    for f in range(FAM):
        leave(f).start()
    for f in range(FAM):
        leave(f).wait()


def families(share, means, out, first, count, limit=None):
    chained = out is not None
    return pl.pallas_call(
        functools.partial(family_kernel, first, count, chained),
        in_specs=[SMEM] + [ANY] * MODELS + [ANY] * (1 if chained else 0),
        out_specs=ANY,
        out_shape=jax.ShapeDtypeStruct((FAM, BAND, DAYS, LAT), BF16),
        input_output_aliases={1 + MODELS: 0} if chained else {},
        scratch_shapes=[
            pltpu.VMEM((MODELS, block_rows(count), DAYS, LANES), BF16),
            pltpu.VMEM((FAM, count, DAYS, LAT), BF16),
            pltpu.SemaphoreType.DMA((MODELS,)),
            pltpu.SemaphoreType.DMA((FAM,)),
        ],
        cost_estimate=pl.CostEstimate(flops=3_000_000 * count, bytes_accessed=170_000 * count, transcendentals=0),
        compiler_params=None if limit is None else grant(limit),
    )(share, *means, *(() if out is None else (out,)))


def moved(array, by):
    return lax.ppermute(array, "group", [(i, (i + by) % MODELS) for i in range(MODELS)])


def from_others(mean):
    return [mean, *(moved(mean, by) for by in (1, -1, 2))]


def exchange(array):
    return lax.all_to_all(array, "tm", split_axis=0, concat_axis=0, tiled=True)


def local(precip, day_bins, family_of):
    sent = pack(precip[0])
    got0, later, day_bins, family_of = lax.optimization_barrier((exchange(sent[0]), sent[1], day_bins, family_of))
    got1 = exchange(later)

    days = jnp.arange(DAYS, dtype=jnp.int32)
    counts = jnp.sum((day_bins[None, :] == days[:, None]).astype(F32), axis=1)
    inverse = 1.0 / jnp.maximum(counts, 1.0)
    scale = jnp.broadcast_to(inverse[:, None], (DAYS, LANES))

    group = lax.axis_index("group")
    turned = (group + jnp.array([0, MODELS - 1, 1, 2], dtype=jnp.int32)) % MODELS
    models = jnp.arange(MODELS, dtype=jnp.int32)
    hot = (family_of[None, :] == jnp.arange(FAM, dtype=jnp.int32)[:, None]).astype(F32)
    members = jnp.maximum(jnp.sum(hot, axis=1), 1.0)
    at = (turned[:, None] == models[None, :]).astype(F32)
    share = jnp.sum(hot[:, None, :] * at[None], axis=2) / members[:, None]

    weight0, total_weight = packed_weight(CHUNKS[0])
    weight1, _ = packed_weight(CHUNKS[1])
    x0 = got0.reshape(TIME, rows_of(CHUNKS[0]), LANES)
    table0, *mean0 = sums(day_bins, inverse, scale, x0, CHUNKS[0])
    means0a = from_others(mean0[0])
    means0b = from_others(mean0[1])
    outs, norm0 = higher(day_bins, x0, table0, scale, jnp.asarray(weight0), STARTS[0], CHUNKS[0])
    first_block, second_block = CHUNKS[0]
    fam = families(share, means0a, None, 0, first_block, LIMITS[0])
    got1, norm0, fam = lax.optimization_barrier((got1, norm0, fam))
    x1 = got1.reshape(TIME, rows_of(CHUNKS[1]), LANES)
    outs, mean1, norm = both(
        day_bins, inverse, scale, x1, jnp.asarray(weight1), norm0, outs, STARTS[1], CHUNKS[1]
    )
    means1 = from_others(mean1)
    parts = lax.all_to_all(norm, ("group", "tm"), split_axis=0, concat_axis=0, tiled=True)
    fam = families(share, means0b, fam, first_block, second_block, LIMITS[1])
    fam = families(share, means1, fam, STARTS[1], CHUNKS[1][0], LIMITS[2])
    parts, fam = lax.optimization_barrier((parts, fam))

    anomaly_norm = jnp.sqrt(jnp.sum(parts.reshape(MODELS, PEERS, TIME), axis=1) / total_weight)
    fields = [o[None].transpose(0, 2, 1, 3) for o in outs]
    return (*fields, fam.transpose(0, 2, 1, 3), anomaly_norm)


def solution(mesh):
    in_specs = (P("group", "tm", None, None), P(), P())
    out_specs = (
        P("group", None, "tm", None),
        P("group", None, "tm", None),
        P("group", None, "tm", None),
        P(None, None, "tm", None),
        P(),
    )
    return jax.shard_map(local, mesh=mesh, in_specs=in_specs, out_specs=out_specs, check_vma=False)
```

```python
import functools
import math

import jax
import jax.numpy as jnp
import numpy as np
from jax import lax
from jax.experimental import pallas as pl
from jax.experimental.pallas import tpu as pltpu
from jax.sharding import PartitionSpec as P


LON = 1440
LAT = 720
DAYS = 16
FAM = 3
MODELS = 4
TIME = 128
LANES = 128
FULL = LAT // LANES
TAIL = LAT - FULL * LANES
HALF = TAIL // 2
PEERS = 32
BAND = LON // PEERS
BLOCK = 8 * BAND
CHUNKS = ((15, 16), (14,))
STARTS = tuple(sum(map(sum, CHUNKS[:c])) for c in range(len(CHUNKS)))

SMEM = pl.BlockSpec(memory_space=pltpu.SMEM)
VMEM = pl.BlockSpec(memory_space=pltpu.VMEM)
ANY = pl.BlockSpec(memory_space=pl.ANY)
STEPS = 8
SEGMENTS = 2
LIMITS = (None, None, 12)
SPAN = TIME // STEPS

F32 = jnp.float32
BF16 = jnp.bfloat16


def tails_of(count):
    return -(-2 * count // 3)


def block_rows(count):
    return FULL * count + tails_of(count)


def rows_of(chunk):
    return -(-sum(map(block_rows, chunk)) // 8) * 8


def blocks_of(chunk):
    lon = row = 0
    for count in chunk:
        yield lon, row, count, tails_of(count), count - tails_of(count)
        lon += count
        row += block_rows(count)


def packed_weight(chunk):
    lat = np.arange(LAT, dtype=np.float64)
    weight = np.cos((-90.0 + (lat + 0.5) * 180.0 / LAT) * (math.pi / 180.0))
    rows = np.zeros((rows_of(chunk), LANES))
    left = weight[FULL * LANES :]
    for _, base, count, tails, split in blocks_of(chunk):
        for j in range(FULL):
            rows[base + j * count : base + (j + 1) * count] = weight[j * LANES : (j + 1) * LANES]
        at = base + FULL * count
        rows[at : at + tails, :TAIL] = left
        for half in range(2):
            part = rows[at + half * split : at + (half + 1) * split]
            part[:, TAIL : TAIL + HALF] = left[half * HALF : (half + 1) * HALF]
    return rows.astype(np.float32), float(weight.sum() * LON)


def loop(length, body, unroll):
    def some(k, carry):
        for i in range(unroll):
            body(k * unroll + i)
        return carry

    lax.fori_loop(0, length // unroll, some, 0)
    for i in range(length - length % unroll, length):
        body(i)


def grant(mebibytes):
    return pltpu.CompilerParams(vmem_limit_bytes=mebibytes * 2**20)


def pack_rows(first, chunk, wide, rows, ready):
    for r in range(8):
        for lon, base, count, tails, split in blocks_of(chunk):
            s = BAND * r + first + lon
            for j in range(FULL):
                rows[base + j * count : base + (j + 1) * count, :] = wide[j, s : s + count, :]
            at = base + FULL * count
            lane = lax.broadcasted_iota(jnp.int32, (split, LANES), 1)
            third = wide[FULL, s + tails : s + count, :]
            for half in range(2):
                own = wide[FULL, s + half * split : s + (half + 1) * split, :]
                moved = pltpu.roll(third, TAIL - half * HALF, 1)
                rows[at + half * split : at + (half + 1) * split, :] = jnp.where(
                    lane < TAIL, own, jnp.where(lane < TAIL + HALF, moved, 0.0)
                )
            if tails > 2 * split:
                own = wide[FULL, s + 2 * split : s + tails, :]
                lane = lax.broadcasted_iota(jnp.int32, own.shape, 1)
                rows[at + 2 * split : at + tails, :] = jnp.where(lane < TAIL, own, 0.0)
        ready[r] = rows[...].astype(BF16)


def pack_kernel(steps, x, *refs):
    n = len(CHUNKS)
    outs, held, ready, wide = refs[:n], refs[n], refs[n + 1 : 2 * n + 1], refs[2 * n + 1]
    rows, got, put = refs[2 * n + 2 : 3 * n + 2], refs[3 * n + 2], refs[3 * n + 3]
    pieces = LON // BLOCK * steps

    def enter(i):
        q, t = i // steps, i % steps
        return pltpu.make_async_copy(x.at[t, pl.ds(pl.multiple_of(q * BLOCK, 8), BLOCK)], held.at[i], got.at[i])

    def leave(c, i):
        q, t = i // steps, i % steps
        return pltpu.make_async_copy(ready[c].at[i], outs[c].at[pl.ds(q * 8, 8), t], put.at[c, i])

    for i in range(pieces):
        enter(i).start()
    for c, chunk in enumerate(CHUNKS):
        total = rows_of(chunk)
        rows[c][total - 8 :, :] = jnp.zeros((8, LANES), F32)

    def piece(i, carry):
        enter(i).wait()
        for j in range(FULL):
            wide[j] = held[i, :, j * LANES : (j + 1) * LANES].astype(F32)
        wide[FULL, :, :TAIL] = held[i, :, FULL * LANES :].astype(F32)
        for c, chunk in enumerate(CHUNKS):
            pack_rows(STARTS[c], chunk, wide, rows[c], ready[c].at[i])
            leave(c, i).start()
        return carry

    lax.fori_loop(0, pieces, piece, 0)
    for c in range(n):
        for i in range(pieces):
            leave(c, i).wait()


def pack(x):
    steps = x.shape[0]
    totals = [rows_of(n) for n in CHUNKS]
    pieces = LON // BLOCK * steps
    return pl.pallas_call(
        functools.partial(pack_kernel, steps),
        in_specs=[ANY],
        out_specs=[ANY] * len(CHUNKS),
        out_shape=[jax.ShapeDtypeStruct((PEERS, steps, total, LANES), BF16) for total in totals],
        scratch_shapes=[pltpu.VMEM((pieces, BLOCK, LAT), BF16)]
        + [pltpu.VMEM((pieces, 8, total, LANES), BF16) for total in totals]
        + [pltpu.VMEM((FULL + 1, BLOCK, LANES), F32)]
        + [pltpu.VMEM((total, LANES), F32) for total in totals]
        + [pltpu.SemaphoreType.DMA((pieces,)), pltpu.SemaphoreType.DMA((len(CHUNKS), pieces))],
        cost_estimate=pl.CostEstimate(flops=10_000_000, bytes_accessed=17_000_000, transcendentals=0),
        name="pack",
    )(x)


def day_rows(table, stride, index):
    halves = [table[pl.ds(8 * h * stride + index, 8, stride=stride), :] for h in range(DAYS // 8)]
    return jnp.concatenate(halves, axis=0)


def unpack_whole(row, outs, block, start, stop):
    first, base, count, _, _ = block

    def whole(i):
        lon = start + i
        for j in range(FULL):
            for out, value in zip(outs, row(base + j * count + lon)):
                out[first + lon, :, j * LANES : (j + 1) * LANES] = value.astype(BF16)

    loop(stop - start, whole, 3)


def unpack_rows(row, outs, block, whole=None):
    first, base, count, tails, split = block
    lane = lax.broadcasted_iota(jnp.int32, (DAYS, LANES), 1)
    at = base + FULL * count

    def tail(lon):
        for out, value in zip(outs, row(at + lon)):
            out[first + lon, :, FULL * LANES :] = value[:, :TAIL].astype(BF16)

    def last(k):
        for out, low, high in zip(outs, row(at + k), row(at + split + k)):
            low = pltpu.roll(low, LANES - TAIL, 1)
            high = pltpu.roll(high, LANES - TAIL + HALF, 1)
            joined = jnp.where(lane < HALF, low, high)
            out[first + tails + k, :, FULL * LANES :] = joined[:, :TAIL].astype(BF16)

    unpack_whole(row, outs, block, 0, count if whole is None else whole)
    loop(tails, tail, 2)
    loop(split, last, 1)


def unpack(table, scale, out, chunk):
    stride = rows_of(chunk) + 1

    def row(index):
        value = day_rows(table, stride, index)
        return [value if scale is None else value * scale]

    for block in blocks_of(chunk):
        unpack_rows(row, [out], block)


def zero(table, stride):
    for d in range(DAYS):
        table[d * stride : (d + 1) * stride, :] = jnp.zeros((stride, LANES), F32)


def add_up(bins, held, mean, total, ready=None):
    stride = total + 1

    def add(t, carry):
        at = bins[t] * stride
        for k in range(total // 8):
            rows = pl.ds(at + 8 * k, 8)
            mean[rows, :] = mean[rows, :] + held[t, 8 * k : 8 * k + 8].astype(F32)
        return carry

    def adds(i, carry):
        if ready is not None:
            ready(i)
        return lax.fori_loop(0, SPAN, lambda t, c: add(i * SPAN + t, c), carry, unroll=4)

    lax.fori_loop(0, STEPS, adds, 0)


def enter(x, held, got, i):
    span = pl.ds(i * SPAN, SPAN)
    return pltpu.make_async_copy(x.at[span], held.at[span], got.at[i])


def divide(inverse, scale, mean, packed, total):
    stride = total + 1
    base = 0
    for rows in packed:

        def one(k, rows=rows, base=base):
            rows[k] = (day_rows(mean, stride, base + k) * scale[...]).astype(BF16)

        loop(rows.shape[0], one, 4)
        base += rows.shape[0]
    for d in range(DAYS):
        rows = slice(d * stride, d * stride + total)
        mean[rows, :] = mean[rows, :] * inverse[d]


def powers(bins, held, mean, second, third, weight, norm, total, ready=None):
    stride = total + 1

    def one(t, carry):
        at = bins[t] * stride
        sums = None
        for k in range(total // 8):
            rows = pl.ds(at + 8 * k, 8)
            tile = slice(8 * k, 8 * k + 8)
            a = held[t, tile].astype(F32) - mean[rows, :]
            q = a * a
            second[rows, :] = second[rows, :] + q
            third[rows, :] = third[rows, :] + q * a
            w = q * weight[tile, :]
            sums = w if sums is None else sums + w
        norm[t] = sums
        return carry

    def some(i, carry):
        if ready is not None:
            ready(i)
        return lax.fori_loop(0, SPAN, lambda t, c: one(i * SPAN + t, c), carry, unroll=2 if total > 100 else 4)

    lax.fori_loop(0, STEPS, some, 0)


def total_norm(norm):
    return jnp.sum(jnp.sum(norm[...], axis=1).T, axis=0, keepdims=True)


def leave(wide, outs, put, first, count, i):
    return pltpu.make_async_copy(wide.at[i], outs[i].at[pl.ds(first, count)], put.at[i])


def sum_kernel(total, bins, inverse, scale, x, mean, *refs):
    packed, held, got = refs[:-2], refs[-2], refs[-1]
    for i in range(STEPS):
        enter(x, held, got, i).start()
    zero(mean, total + 1)
    add_up(bins, held, mean, total, lambda i: enter(x, held, got, i).wait())
    divide(inverse, scale, mean, packed, total)


def table_shape(total):
    return (DAYS * (total + 1), LANES)


def row_shape(total):
    return jax.ShapeDtypeStruct((total, DAYS, LANES), BF16)


def sums(bins, inverse, scale, x, chunk):
    total = rows_of(chunk)
    return pl.pallas_call(
        functools.partial(sum_kernel, total),
        in_specs=[SMEM, SMEM, VMEM, ANY],
        out_specs=[VMEM] * (1 + len(chunk)),
        out_shape=[jax.ShapeDtypeStruct(table_shape(total), F32)] + [row_shape(block_rows(n)) for n in chunk],
        scratch_shapes=[pltpu.VMEM((TIME, total, LANES), BF16), pltpu.SemaphoreType.DMA((STEPS,))],
        cost_estimate=pl.CostEstimate(flops=3_000_000 * sum(chunk), bytes_accessed=230_000 * sum(chunk), transcendentals=0),
        name="sums",
    )(bins, inverse, scale, x)


def power_kernel(first, chunk, bins, x, mean, scale, weight, *refs):
    outs, (after, held, second, third, norm, wide, got, put) = refs[:3], refs[3:]
    total = rows_of(chunk)
    count = sum(chunk)
    for i in range(STEPS):
        enter(x, held, got, i).start()
    zero(second, total + 1)
    zero(third, total + 1)
    unpack(mean, None, wide.at[0], chunk)
    leave(wide, outs, put, first, count, 0).start()
    powers(
        bins, held, mean, second, third, weight, norm, total, lambda i: enter(x, held, got, i).wait()
    )
    after[...] = total_norm(norm)
    for i, table in ((1, second), (2, third)):
        unpack(table, scale[...], wide.at[i], chunk)
        leave(wide, outs, put, first, count, i).start()
    for i in range(3):
        leave(wide, outs, put, first, count, i).wait()


FIELD = jax.ShapeDtypeStruct((BAND, DAYS, LAT), BF16)


def higher(bins, x, mean, scale, weight, first, chunk):
    total = rows_of(chunk)
    result = pl.pallas_call(
        functools.partial(power_kernel, first, chunk),
        in_specs=[SMEM, ANY] + [VMEM] * 3,
        out_specs=[ANY] * 3 + [VMEM],
        out_shape=[FIELD] * 3 + [jax.ShapeDtypeStruct((1, TIME), F32)],
        scratch_shapes=[
            pltpu.VMEM((TIME, total, LANES), BF16),
            pltpu.VMEM(table_shape(total), F32),
            pltpu.VMEM(table_shape(total), F32),
            pltpu.VMEM((TIME, 8, LANES), F32),
            pltpu.VMEM((3, sum(chunk), DAYS, LAT), BF16),
            pltpu.SemaphoreType.DMA((STEPS,)),
            pltpu.SemaphoreType.DMA((3,)),
        ],
        cost_estimate=pl.CostEstimate(flops=13_000_000 * sum(chunk), bytes_accessed=330_000 * sum(chunk), transcendentals=0),
        name="higher",
    )(bins, x, mean, scale, weight)
    return result[:3], result[3]


def both_kernel(first, chunk, bins, inverse, scale, x, weight, before, *refs):
    outs, (packed, after, mean, second, third, norm, wide, put) = refs[3:6], refs[6:]
    total = rows_of(chunk)
    count = sum(chunk)
    for table in (mean, second, third):
        zero(table, total + 1)
    add_up(bins, x, mean, total)
    divide(inverse, scale, mean, (packed,), total)
    (block,) = blocks_of(chunk)
    unpack_rows(lambda i: [packed[i].astype(F32)], [wide.at[0]], block)
    leave(wide, outs, put, first, count, 0).start()
    powers(bins, x, mean, second, third, weight, norm, total)
    row = before[...] + total_norm(norm)
    after[:, 0, :] = jnp.broadcast_to(row, (MODELS * PEERS, TIME))
    for i, table in ((1, second), (2, third)):
        unpack(table, scale[...], wide.at[i], chunk)
        leave(wide, outs, put, first, count, i).start()
    for i in range(3):
        leave(wide, outs, put, first, count, i).wait()


def both(bins, inverse, scale, x, weight, before, outs, first, chunk):
    total = rows_of(chunk)
    result = pl.pallas_call(
        functools.partial(both_kernel, first, chunk),
        in_specs=[SMEM, SMEM, VMEM, VMEM, VMEM, VMEM] + [ANY] * 3,
        out_specs=[ANY] * 3 + [VMEM] * 2,
        out_shape=[FIELD] * 3 + [row_shape(block_rows(*chunk)), jax.ShapeDtypeStruct((MODELS * PEERS, 1, TIME), F32)],
        input_output_aliases={6: 0, 7: 1, 8: 2},
        scratch_shapes=[
            pltpu.VMEM(table_shape(total), F32),
            pltpu.VMEM(table_shape(total), F32),
            pltpu.VMEM(table_shape(total), F32),
            pltpu.VMEM((TIME, 8, LANES), F32),
            pltpu.VMEM((3, sum(chunk), DAYS, LAT), BF16),
            pltpu.SemaphoreType.DMA((3,)),
        ],
        cost_estimate=pl.CostEstimate(flops=16_000_000 * sum(chunk), bytes_accessed=330_000 * sum(chunk), transcendentals=0),
        name="both",
        compiler_params=grant(24),
    )(bins, inverse, scale, x, weight, before, *outs)
    return result[:3], result[3], result[4]


def family_kernel(first, count, chained, near, share, *refs):
    means = refs[:MODELS]
    out, wide, put, *refs = refs[MODELS + (1 if chained else 0) :]
    held, got = refs or (means, None)

    def enter(k):
        return pltpu.make_async_copy(means[k], held.at[k], got.at[k])

    cuts = [count * i // SEGMENTS for i in range(SEGMENTS + 1)]

    def leave(i):
        span = cuts[i + 1] - cuts[i]
        return pltpu.make_async_copy(
            wide.at[:, pl.ds(cuts[i], span)], out.at[:, pl.ds(first + cuts[i], span)], put.at[i]
        )

    if not near:
        for k in range(MODELS):
            enter(k).start()
        for k in range(MODELS):
            enter(k).wait()
    shares = [[share[f, k] for k in range(MODELS)] for f in range(FAM)]

    def row(index):
        values = [(held[k][index] if near else held[k, index]).astype(F32) for k in range(MODELS)]
        results = []
        for f in range(FAM):
            value = values[0] * shares[f][0]
            for k in range(1, MODELS):
                value = value + values[k] * shares[f][k]
            results.append(value)
        return results

    (block,) = blocks_of((count,))
    outs = [wide.at[f] for f in range(FAM)]
    unpack_rows(row, outs, block, 0)
    for i in range(SEGMENTS):
        unpack_whole(row, outs, block, cuts[i], cuts[i + 1])
        leave(i).start()
    for i in range(SEGMENTS):
        leave(i).wait()


def families(share, means, out, first, count, limit=None):
    chained = out is not None
    near = limit is not None
    return pl.pallas_call(
        functools.partial(family_kernel, first, count, chained, near),
        in_specs=[SMEM] + [VMEM if near else ANY] * MODELS + [ANY] * (1 if chained else 0),
        out_specs=ANY,
        out_shape=jax.ShapeDtypeStruct((FAM, BAND, DAYS, LAT), BF16),
        input_output_aliases={1 + MODELS: 0} if chained else {},
        scratch_shapes=[pltpu.VMEM((FAM, count, DAYS, LAT), BF16), pltpu.SemaphoreType.DMA((SEGMENTS,))]
        + (
            []
            if near
            else [pltpu.VMEM((MODELS, block_rows(count), DAYS, LANES), BF16), pltpu.SemaphoreType.DMA((MODELS,))]
        ),
        cost_estimate=pl.CostEstimate(flops=3_000_000 * count, bytes_accessed=170_000 * count, transcendentals=0),
        compiler_params=None if limit is None else grant(limit),
    )(share, *means, *(() if out is None else (out,)))


def moved(array, by):
    return lax.ppermute(array, "group", [(i, (i + by) % MODELS) for i in range(MODELS)])


def from_others(mean):
    across = moved(mean, 2)
    return [mean, moved(mean, 1), moved(mean, -1), across]


def exchange(array):
    return lax.all_to_all(array, "tm", split_axis=0, concat_axis=0, tiled=True)


def local(precip, day_bins, family_of):
    sent = pack(precip[0])
    got0, later, day_bins, family_of = lax.optimization_barrier((exchange(sent[0]), sent[1], day_bins, family_of))
    got1 = exchange(later)

    days = jnp.arange(DAYS, dtype=jnp.int32)
    counts = jnp.sum((day_bins[None, :] == days[:, None]).astype(F32), axis=1)
    inverse = 1.0 / jnp.maximum(counts, 1.0)
    scale = jnp.broadcast_to(inverse[:, None], (DAYS, LANES))

    group = lax.axis_index("group")
    turned = (group + jnp.array([0, MODELS - 1, 1, 2], dtype=jnp.int32)) % MODELS
    models = jnp.arange(MODELS, dtype=jnp.int32)
    hot = (family_of[None, :] == jnp.arange(FAM, dtype=jnp.int32)[:, None]).astype(F32)
    members = jnp.maximum(jnp.sum(hot, axis=1), 1.0)
    at = (turned[:, None] == models[None, :]).astype(F32)
    share = jnp.sum(hot[:, None, :] * at[None], axis=2) / members[:, None]

    weight0, total_weight = packed_weight(CHUNKS[0])
    weight1, _ = packed_weight(CHUNKS[1])
    x0 = got0.reshape(TIME, rows_of(CHUNKS[0]), LANES)
    table0, *mean0 = sums(day_bins, inverse, scale, x0, CHUNKS[0])
    means0a = from_others(mean0[0])
    means0b = from_others(mean0[1])
    outs, norm0 = higher(day_bins, x0, table0, scale, jnp.asarray(weight0), STARTS[0], CHUNKS[0])
    first_block, second_block = CHUNKS[0]
    fam = families(share, means0a, None, 0, first_block, LIMITS[0])
    got1, norm0, fam = lax.optimization_barrier((got1, norm0, fam))
    x1 = got1.reshape(TIME, rows_of(CHUNKS[1]), LANES)
    outs, mean1, norm = both(
        day_bins, inverse, scale, x1, jnp.asarray(weight1), norm0, outs, STARTS[1], CHUNKS[1]
    )
    means1 = from_others(mean1)
    parts = lax.all_to_all(norm, ("group", "tm"), split_axis=0, concat_axis=0, tiled=True)
    fam = families(share, means0b, fam, first_block, second_block, LIMITS[1])
    fam = families(share, means1, fam, STARTS[1], CHUNKS[1][0], LIMITS[2])
    parts, fam = lax.optimization_barrier((parts, fam))

    anomaly_norm = jnp.sqrt(jnp.sum(parts.reshape(MODELS, PEERS, TIME), axis=1) / total_weight)
    fields = [o[None].transpose(0, 2, 1, 3) for o in outs]
    return (*fields, fam.transpose(0, 2, 1, 3), anomaly_norm)


def solution(mesh):
    in_specs = (P("group", "tm", None, None), P(), P())
    out_specs = (
        P("group", None, "tm", None),
        P("group", None, "tm", None),
        P("group", None, "tm", None),
        P(None, None, "tm", None),
        P(),
    )
    return jax.shard_map(local, mesh=mesh, in_specs=in_specs, out_specs=out_specs, check_vma=False)
```
